32 devices in a mesh: seg: 16 (over z, y, x), slab: 2 (over core).
Axes of the slice: x: 2, y: 2, z: 4, core: 2. Of those that a mesh axis runs over, the one named last changes fastest.
Arguments:
- block: float32 [16, 4, 16, 4096], P('seg', None, 'slab'), may hold values from -6 to 6
- base_velocity: bfloat16 [16, 8, 2, 16, 4096], P('seg', None, None, 'slab'), may hold values from -6 to 6
Outputs:
- new_block: float32 [16, 4, 16, 4096], P('seg', None, 'slab')
The draws below stay inside these ranges and needn't reach their ends.
All inputs are finite; a program needn't handle non-finite values.
Results may differ from the reference program's by a relative error of at most 0.0003.
Values may be sent and summed in bfloat16 or wider, within the bound.
No kernel may reach another device: no remote copies, remote signals or barrier semaphores. Data moves between devices by JAX's collectives and lax.ppermute only.
A program may use at most 64 MiB of HBM per device.

```python
import jax
import jax.numpy as jnp
from jax import lax

NXW = 4096
STEPS = 8
HOPS = 4
NVEC = 4
SEGMENTS = 16
NY = 16


def level_of(rng, shape, split, low, largest):
    def one(axis_at, shards_of):
        steps = jax.random.uniform(jax.random.fold_in(jax.random.fold_in(rng, 6), axis_at), (shards_of,), jnp.float32, low / len(split), largest / len(split))
        return jnp.repeat(jnp.exp(steps), shape[axis_at] // shards_of).reshape((-1,) + (1,) * (len(shape) - axis_at - 1))

    level = one(*split[0])
    for cut in split[1:]:
        level = level * one(*cut)
    return level


def bell_draw(key, shape, width, most, split=(), kind=jnp.bfloat16):
    array = width * jax.random.normal(key, shape, jnp.float32)
    if split:
        array = array * level_of(key, shape, split, -0.22, 0.18)
    return jnp.clip(array, -most, most).astype(kind)


def setup_inputs(seed: int = 0) -> dict:
    key_list = jax.random.split(jax.random.key(seed), 3)
    return {
        "block": bell_draw(key_list[0], (SEGMENTS, NVEC, NY, NXW), 1.0, 6.0, ((0, 16), (2, 2)), jnp.float32),
        "base_velocity": bell_draw(key_list[1], (SEGMENTS, STEPS, 2, NY, NXW), 1.0, 6.0, ((0, 16), (3, 2))),
    }


def advance_full(field, velocity):
    up = jnp.roll(field, -1, 1)
    down = jnp.roll(field, 1, 1)
    east = jnp.roll(field, -1, 2)
    west = jnp.roll(field, 1, 2)
    speed_x = velocity[0].astype(jnp.float32)
    speed_y = velocity[1].astype(jnp.float32)
    return field + 0.2 * (up + down + east + west - 4.0 * field) - 0.05 * (speed_x * (east - west) + speed_y * (up - down)) - 0.02 * field

def lower_inverse(lower):
    count = lower.shape[0]
    rows = []
    for i in range(count):
        entries = []
        for j in range(count):
            if j > i:
                entries.append(jnp.zeros((), jnp.float32))
            elif j == i:
                entries.append(1.0 / lower[i, i])
            else:
                total = jnp.zeros((), jnp.float32)
                for k in range(j, i):
                    total = total + lower[i, k] * rows[k][j]
                entries.append(-total / lower[i, i])
        rows.append(entries)
    return jnp.stack([jnp.stack(r) for r in rows])

def reference(block, base_velocity):

    def propagate(pair):
        vectors, velocity = pair
        for j in range(STEPS):
            vectors = advance_full(vectors, velocity[j])
        return vectors
    for hop in range(HOPS):
        moved = lax.map(propagate, (block, base_velocity))
        residual = jnp.roll(moved, 1, 0) - block
        gram = jnp.einsum('sayx,sbyx->ab', residual, residual, precision=lax.Precision.HIGHEST)
        inverse = lower_inverse(jnp.linalg.cholesky(gram))
        block = jnp.einsum('ab,sbyx->sayx', inverse, residual, precision=lax.Precision.HIGHEST)
    return block
```

```python
import functools

import jax
import jax.numpy as jnp
from jax import lax
from jax.experimental import pallas as pl
from jax.experimental.pallas import tpu as pltpu
from jax.sharding import PartitionSpec as P

HOPS = 4
SUB = 8
LANE = 128
VMEM = pl.BlockSpec(memory_space=pltpu.VMEM)


def tiled(rows):
    lead, (height, width) = rows.shape[:-2], rows.shape[-2:]
    cut = rows.reshape(lead + (height, width // LANE, LANE))
    return jnp.swapaxes(cut, -3, -2)


def untiled(tiles):
    lead, (count, height, lane) = tiles.shape[:-3], tiles.shape[-3:]
    return jnp.swapaxes(tiles, -3, -2).reshape(lead + (height, count * lane))


def propagate_kernel(pieces, index, subtract, keep, apart, *refs):
    def take(count):
        nonlocal refs
        taken, refs = refs[:count], refs[count:]
        return taken

    def pick(group, piece):
        return group[piece].at[0] if len(group) > 1 or pieces == 1 else group[0].at[piece]

    velocity = take(pieces)
    if subtract:
        previous, arrived = take(1), take(1)
        start_out = take(pieces if apart else 1)
    else:
        previous = take(pieces)
    moved = take(keep if apart else 1)
    ping, pong = refs
    depth, _, columns, height, _ = velocity[0].shape
    rows = pieces * height
    lane = lax.broadcasted_iota(jnp.int32, (SUB, LANE), 1)
    first, last = lane == 0, lane == LANE - 1
    blocks = range(rows // SUB)

    def place(ref, j, b, value):
        ref[j, pl.ds(SUB + SUB * b, SUB), :] = value
        if b == blocks[0]:
            ref[j, pl.ds(SUB + rows, 1), :] = value[:1]
        if b == blocks[-1]:
            ref[j, pl.ds(SUB - 1, 1), :] = value[SUB - 1 :]

    for j in range(columns):
        for b in blocks:
            piece, at = divmod(SUB * b, height)
            at = pl.ds(at, SUB)
            if subtract:
                value = pick(arrived, piece)[j, at, :] - pick(previous, piece)[j, at, :]
                pick(start_out, piece)[j, at, :] = value
            else:
                value = previous[piece][index, j, at, :]
            place(ping, j, b, value)

    def step(k, source, write):
        for b in blocks:
            piece, at = divmod(SUB * b, height)
            rows_at = pl.ds(SUB + SUB * b, SUB)
            here = [source[j % columns, rows_at, :] for j in (-1, 0, 1)]
            for j in range(columns):
                left, centre, right = here
                west = pltpu.roll(jnp.where(last, left, centre), 1, 1)
                east = pltpu.roll(jnp.where(first, right, centre), LANE - 1, 1)
                up = source[j, pl.ds(SUB + 1 + SUB * b, SUB), :]
                down = source[j, pl.ds(SUB - 1 + SUB * b, SUB), :]
                speed_x = velocity[piece][k, 0, j, pl.ds(at, SUB), :].astype(jnp.float32)
                speed_y = velocity[piece][k, 1, j, pl.ds(at, SUB), :].astype(jnp.float32)
                carried = speed_x * (west - east) + speed_y * (down - up)
                write(j, b, 0.9 * centre + ((west + east) + (up + down)) + 0.25 * carried)
                here = [centre, right, source[(j + 2) % columns, rows_at, :]]

    def pair(i, carry):
        step(2 * i, ping, functools.partial(place, pong))
        step(2 * i + 1, pong, functools.partial(place, ping))
        return carry

    lax.fori_loop(0, (depth - 1) // 2, pair, 0)
    source = ping
    if depth % 2 == 0:
        step(depth - 2, ping, functools.partial(place, pong))
        source = pong
    scale = 0.2**depth

    def finish(j, b, value):
        piece, at = divmod(SUB * b, height)
        if piece < keep:
            pick(moved, piece)[j, pl.ds(at, SUB), :] = scale * value

    step(depth - 1, source, finish)


def propagate(velocity, previous, index=0, arrived=None, keep=None, apart=False):
    pieces = len(velocity)
    keep = pieces if keep is None else keep
    _, _, columns, height, lane = velocity[0].shape

    def shapes(count):
        parts = [1] * count if apart else [count]
        return [jax.ShapeDtypeStruct((n, columns, height, lane), jnp.float32) for n in parts]

    subtract = arrived is not None
    outs = (shapes(pieces) if subtract else []) + shapes(keep)
    scratch = pltpu.VMEM((columns, pieces * height + 2 * SUB, lane), jnp.float32)
    args = [*velocity] + ([previous, arrived] if subtract else [*previous])
    out = pl.pallas_call(
        functools.partial(propagate_kernel, pieces, index, subtract, keep, apart),
        out_shape=outs,
        in_specs=[VMEM] * len(args),
        out_specs=[VMEM] * len(outs),
        scratch_shapes=[scratch, scratch],
        compiler_params=pltpu.CompilerParams(vmem_limit_bytes=16 << 20),
        name="propagate",
    )(*args)
    if apart:
        return out[:pieces], out[pieces:]
    return out if subtract else out[0]


def gram_kernel(arrived_count, *refs):
    base = refs[0]
    groups = [(refs[1 + i], refs[1 + arrived_count + i]) for i in range(arrived_count)]
    residual, gram = refs[1 + 2 * arrived_count :]
    count, columns, height, _ = residual.shape
    size = [a.shape[0] for a, _ in groups]
    shift = base[0]
    sums = {}
    for j in range(columns):
        for at in range(0, height, SUB):
            values = []
            for (a, s), n in zip(groups, size):
                for i in range(n):
                    values.append(a[i, j, pl.ds(at, SUB), :] - s[i, j, pl.ds(at, SUB), :])
            for p in range(count):
                residual[p, j, pl.ds(at, SUB), :] = values[p]
                for q in range(p + 1):
                    term = values[p] * values[q]
                    sums[p, q] = term if (p, q) not in sums else sums[p, q] + term
    for (p, q), total in sums.items():
        line = jnp.sum(total, axis=0, keepdims=True)
        a, b = lax.rem(shift + p, count), lax.rem(shift + q, count)
        gram[pl.ds(a * count + b, 1), :] = line
        if p != q:
            gram[pl.ds(b * count + a, 1), :] = line


def local_gram(shift, arrived, start):
    count = sum(a.shape[0] for a in arrived)
    shape = (count,) + arrived[0].shape[1:]
    return pl.pallas_call(
        functools.partial(gram_kernel, len(arrived)),
        out_shape=[jax.ShapeDtypeStruct(shape, jnp.float32), jax.ShapeDtypeStruct((count * count, LANE), jnp.float32)],
        in_specs=[pl.BlockSpec(memory_space=pltpu.SMEM)] + [VMEM] * (2 * len(arrived)),
        out_specs=[VMEM, VMEM],
        compiler_params=pltpu.CompilerParams(vmem_limit_bytes=16 << 20),
        name="gram",
    )(shift, *arrived, *start)


def solve_kernel(base, gram, residual, out):
    count, columns, height, lane = residual.shape
    total = jnp.sum(gram[...], axis=1, keepdims=True)
    entry = lambda a, b: total[a * count + b : a * count + b + 1, :]
    lower, inverse = {}, {}
    for a in range(count):
        for b in range(a + 1):
            value = entry(a, b)
            for k in range(b):
                value = value - lower[a, k] * lower[b, k]
            lower[a, b] = jnp.sqrt(value) if a == b else value / lower[b, b]
    for a in range(count):
        inverse[a, a] = 1.0 / lower[a, a]
        for b in range(a):
            value = lower[a, b] * inverse[b, b]
            for k in range(b + 1, a):
                value = value + lower[a, k] * inverse[k, b]
            inverse[a, b] = -value / lower[a, a]
    factors = {at: jnp.broadcast_to(value, (SUB, lane)) for at, value in inverse.items()}
    place = [lax.rem(a + count - base[0], count) for a in range(count)]
    for j in range(columns):
        for at in range(0, height, SUB):
            values = [residual[place[a], j, pl.ds(at, SUB), :] for a in range(count)]
            for a in range(count):
                value = factors[a, 0] * values[0]
                for b in range(1, a + 1):
                    value = value + factors[a, b] * values[b]
                out[a, j, pl.ds(at, SUB), :] = value


def solved(shift, gram, residual):
    return pl.pallas_call(
        solve_kernel,
        out_shape=jax.ShapeDtypeStruct(residual.shape, jnp.float32),
        in_specs=[pl.BlockSpec(memory_space=pltpu.SMEM), VMEM, VMEM],
        out_specs=VMEM,
        compiler_params=pltpu.CompilerParams(vmem_limit_bytes=16 << 20),
        name="solve",
    )(shift, gram, residual)


def summed(value, axes):
    count = 1
    for axis in axes:
        count *= lax.axis_size(axis)
    if count & (count - 1):
        return lax.psum(value, axes)
    distance = 1
    while distance < count:
        value = value + lax.ppermute(value, axes, [(i, i ^ distance) for i in range(count)])
        distance *= 2
    return value


def from_slab(value, distance):
    size = lax.axis_size("slab")
    return lax.ppermute(value, "slab", [((i + distance) % size, i) for i in range(size)])


def to_next(value, turn=0):
    segs, slabs = lax.axis_size("seg"), lax.axis_size("slab")
    route = []
    for s in range(segs):
        for c in range(slabs):
            route.append((s * slabs + c, (s + 1) % segs * slabs + (c + turn) % slabs))
    return lax.ppermute(value, ("seg", "slab"), route)


def split_vectors(vectors, velocity):
    slabs, mine = lax.axis_size("slab"), lax.axis_index("slab")
    share = vectors.shape[0] // slabs

    def part(distance):
        at = lax.rem(mine + distance, slabs) * share
        return lax.dynamic_slice_in_dim(vectors, at, share, 0)

    start, speeds = [part(0)], [velocity]
    for d in range(1, slabs):
        start.append(from_slab(part(slabs - d), d))
        speeds.append(from_slab(velocity, d))
    moved = [propagate(speeds, start, i) for i in range(share)]
    previous = [jnp.concatenate([part[i : i + 1] for part in start], 0) for i in range(share)]
    for hop in range(1, HOPS):
        for i in range(share):
            final = hop + 1 == HOPS
            previous[i], moved[i] = propagate(speeds, previous[i], 0, to_next(moved[i]), None, final)
    arrived, begun = [], []
    for d in range(slabs):
        for i in range(share):
            at = (slabs - d) % slabs
            arrived.append(to_next(moved[i][at], at))
            begun.append(from_slab(previous[i][at], d) if d else previous[i][0])
    shift = jnp.full((1,), mine * share, jnp.int32)
    return shift, arrived, begun


def split_rows(vectors, velocity):
    depth, height = velocity.shape[0], vectors.shape[2]

    def pieces(value):
        after = value[..., :depth, :]
        before = value[..., height - depth :, :]
        return [value, from_slab(after, 1), from_slab(before, -1)]

    speeds = pieces(velocity)
    begun = vectors
    for hop in range(HOPS):
        state = pieces(begun)
        arrived = [to_next(propagate(speeds, state, i, keep=1)) for i in range(vectors.shape[0])]
        if hop + 1 < HOPS:
            begun = jnp.concatenate(arrived, 0) - begun
    return jnp.zeros((1,), jnp.int32), arrived, [begun[i : i + 1] for i in range(vectors.shape[0])]


def shards(block, base_velocity):
    vectors, velocity = tiled(block[0]), tiled(base_velocity[0])
    even = vectors.shape[0] % lax.axis_size("slab") == 0
    shift, arrived, begun = (split_vectors if even else split_rows)(vectors, velocity)
    residual, gram = local_gram(shift, arrived, begun)
    gram = summed(gram, ("seg", "slab"))
    return untiled(solved(shift, gram, residual))[None]


def solution(mesh):
    placed = (P("seg", None, "slab", None), P("seg", None, None, "slab", None))
    return jax.shard_map(
        shards, mesh=mesh, in_specs=placed, out_specs=P("seg", None, "slab", None), check_vma=False
    )
```

```python
import functools

import jax
import jax.numpy as jnp
from jax import lax
from jax.experimental import pallas as pl
from jax.experimental.pallas import tpu as pltpu
from jax.sharding import PartitionSpec as P

HOPS = 4
SUB = 8
LANE = 128
VMEM = pl.BlockSpec(memory_space=pltpu.VMEM)


def tiled(rows):
    lead, (height, width) = rows.shape[:-2], rows.shape[-2:]
    cut = rows.reshape(lead + (height, width // LANE, LANE))
    return jnp.swapaxes(cut, -3, -2)


def untiled(tiles):
    lead, (count, height, lane) = tiles.shape[:-3], tiles.shape[-3:]
    return jnp.swapaxes(tiles, -3, -2).reshape(lead + (height, count * lane))


def advance(velocity, ping, pong, pieces):
    depth, _, columns, height, _ = velocity[0].shape
    rows = pieces * height
    lane = lax.broadcasted_iota(jnp.int32, (SUB, LANE), 1)
    first, last = lane == 0, lane == LANE - 1

    def step(k, source, target):
        for b in range(rows // SUB):
            piece, at = divmod(SUB * b, height)
            rows_at = pl.ds(SUB + SUB * b, SUB)
            here = [source[j % columns, rows_at, :] for j in (-1, 0, 1)]
            for j in range(columns):
                left, centre, right = here
                west = pltpu.roll(jnp.where(last, left, centre), 1, 1)
                east = pltpu.roll(jnp.where(first, right, centre), LANE - 1, 1)
                up = source[j, pl.ds(SUB + 1 + SUB * b, SUB), :]
                down = source[j, pl.ds(SUB - 1 + SUB * b, SUB), :]
                speed_x = velocity[piece][k, 0, j, pl.ds(at, SUB), :].astype(jnp.float32)
                speed_y = velocity[piece][k, 1, j, pl.ds(at, SUB), :].astype(jnp.float32)
                carried = speed_x * (west - east) + speed_y * (down - up)
                place(target, rows, j, b, 0.9 * centre + ((west + east) + (up + down)) + 0.25 * carried)
                here = [centre, right, source[(j + 2) % columns, rows_at, :]]

    def pair(i, carry):
        step(2 * i, ping, pong)
        step(2 * i + 1, pong, ping)
        return carry

    lax.fori_loop(0, depth // 2, pair, 0)
    if depth % 2:
        step(depth - 1, ping, pong)
        return pong
    return ping


def place(ref, rows, j, b, value):
    ref[j, pl.ds(SUB + SUB * b, SUB), :] = value
    if b == 0:
        ref[j, pl.ds(SUB + rows, 1), :] = value[:1]
    if b == rows // SUB - 1:
        ref[j, pl.ds(SUB - 1, 1), :] = value[SUB - 1 :]


def tiles_of(pieces, columns, height):
    for j in range(columns):
        for b in range(pieces * height // SUB):
            piece, at = divmod(SUB * b, height)
            yield piece, j, pl.ds(at, SUB), b, (piece * columns + j) * (height // SUB) + at // SUB


TOP = 13.0


def propagate_kernel(pieces, index, first, final, *refs):
    refs = list(refs)
    take = lambda count: [refs.pop(0) for _ in range(count)]
    velocity = take(pieces)
    depth, _, columns, height, _ = velocity[0].shape
    rows, count = pieces * height, pieces * columns * height // SUB
    if first:
        previous = take(pieces)
    else:
        previous, message, missed = take(3)
        start = take(pieces) if final else take(1)
    if final:
        moved = take(pieces)
    else:
        sent, error = take(2)
    ping, pong = refs

    if not first:
        back = jnp.exp2(message[count] - TOP)
    for piece, j, at, b, m in tiles_of(pieces, columns, height):
        if first:
            value = previous[piece][index, j, at, :]
        else:
            value = message[m] * back - previous[piece, j, at, :]
            if final:
                start[piece][0, j, at, :] = value
            else:
                start[0][piece, j, at, :] = value
        place(ping, rows, j, b, value)

    done = advance(velocity, ping, pong, pieces)
    largest = None
    for piece, j, at, b, m in tiles_of(pieces, columns, height):
        value = 0.2**depth * done[j, pl.ds(SUB + SUB * b, SUB), :]
        if not first:
            value = value + missed[m]
        if final:
            moved[piece][0, j, at, :] = value
        else:
            sent[m] = value
            size = jnp.abs(value)
            largest = size if largest is None else jnp.maximum(largest, size)
    if final:
        return
    largest = jnp.broadcast_to(jnp.max(largest, axis=(0, 1), keepdims=True), (SUB, LANE))
    power = jnp.clip(jnp.floor(jnp.log2(largest)), -100.0, 100.0)
    scale, back = jnp.exp2(TOP - power), jnp.exp2(power - TOP)
    sent[count] = power
    for m in range(count):
        value = sent[m]
        scaled = value * scale
        wide = scaled * 8193.0
        short = wide - (wide - scaled)
        sent[m] = short
        error[m] = short * back - value


@functools.partial(jax.jit, static_argnames=("index", "final"))
def propagate(velocity, state, index=0, final=False):
    pieces = len(velocity)
    _, _, columns, height, lane = velocity[0].shape
    count = pieces * columns * height // SUB
    first = isinstance(state, list)
    shape = lambda *s: jax.ShapeDtypeStruct(s + (lane,), jnp.float32)
    parts = [shape(1, columns, height)] * pieces
    outs = [] if first else (parts if final else [shape(pieces, columns, height)])
    outs = outs + (parts if final else [shape(count + 1, SUB), shape(count, SUB)])
    scratch = pltpu.VMEM((columns, pieces * height + 2 * SUB, lane), jnp.float32)
    args = [*velocity, *state]
    out = pl.pallas_call(
        functools.partial(propagate_kernel, pieces, index, first, final),
        out_shape=outs,
        in_specs=[VMEM] * len(args),
        out_specs=[VMEM] * len(outs),
        scratch_shapes=[scratch, scratch],
        compiler_params=pltpu.CompilerParams(vmem_limit_bytes=16 << 20),
        name="propagate",
    )(*args)
    return (out[:pieces], out[pieces:]) if final else out


def rows_kernel(pieces, index, *refs):
    velocity, previous, (moved, ping, pong) = refs[:pieces], refs[pieces : 2 * pieces], refs[2 * pieces :]
    depth, _, columns, height, _ = velocity[0].shape
    for piece, j, at, b, _ in tiles_of(pieces, columns, height):
        place(ping, pieces * height, j, b, previous[piece][index, j, at, :])
    done = advance(velocity, ping, pong, pieces)
    for piece, j, at, b, _ in tiles_of(1, columns, height):
        moved[0, j, at, :] = 0.2**depth * done[j, pl.ds(SUB + SUB * b, SUB), :]


@functools.partial(jax.jit, static_argnames=("index",))
def propagate_rows(velocity, state, index):
    pieces = len(velocity)
    _, _, columns, height, lane = velocity[0].shape
    scratch = pltpu.VMEM((columns, pieces * height + 2 * SUB, lane), jnp.float32)
    return pl.pallas_call(
        functools.partial(rows_kernel, pieces, index),
        out_shape=jax.ShapeDtypeStruct((1, columns, height, lane), jnp.float32),
        in_specs=[VMEM] * (2 * pieces),
        out_specs=VMEM,
        scratch_shapes=[scratch, scratch],
        compiler_params=pltpu.CompilerParams(vmem_limit_bytes=16 << 20),
        name="propagate_rows",
    )(*velocity, *state)


def gram_kernel(groups, *refs):
    base, refs = refs[0], refs[1:]
    arrived, start = refs[:groups], refs[groups : 2 * groups]
    residual, gram, lines = refs[2 * groups :]
    count, columns, height, _ = residual.shape
    sums = {}
    for j in range(columns):
        for at in range(0, height, SUB):
            values = []
            for a, s in zip(arrived, start):
                for i in range(a.shape[0]):
                    values.append(a[i, j, pl.ds(at, SUB), :] - s[i, j, pl.ds(at, SUB), :])
            for p in range(count):
                residual[p, j, pl.ds(at, SUB), :] = values[p]
                for q in range(p + 1):
                    term = values[p] * values[q]
                    sums[p, q] = term if (p, q) not in sums else sums[p, q] + term
    for (p, q), total in sums.items():
        line = jnp.sum(total, axis=0, keepdims=True)
        a, b = lax.rem(base[0] + p, count), lax.rem(base[0] + q, count)
        lines[pl.ds(a * count + b, 1), :] = line
        if p != q:
            lines[pl.ds(b * count + a, 1), :] = line
    totals = jnp.where(diagonal(count), jnp.sum(lines[...], axis=1, keepdims=True), 0.0)
    gram[...] = jnp.broadcast_to(jnp.sum(totals, axis=0, keepdims=True), gram.shape)


def diagonal(count):
    shape = (count * count, LANE)
    return lax.broadcasted_iota(jnp.int32, shape, 0) == lax.broadcasted_iota(jnp.int32, shape, 1)


def local_gram(shift, arrived, start, copies):
    count = sum(a.shape[0] for a in arrived)
    shape = (count,) + arrived[0].shape[1:]
    return pl.pallas_call(
        functools.partial(gram_kernel, len(arrived)),
        out_shape=[jax.ShapeDtypeStruct(shape, jnp.float32), jax.ShapeDtypeStruct((copies, LANE), jnp.float32)],
        in_specs=[pl.BlockSpec(memory_space=pltpu.SMEM)] + [VMEM] * (2 * len(arrived)),
        out_specs=[VMEM, VMEM],
        scratch_shapes=[pltpu.VMEM((count * count, LANE), jnp.float32)],
        compiler_params=pltpu.CompilerParams(vmem_limit_bytes=16 << 20),
        name="gram",
    )(shift, *arrived, *start)


def solve_kernel(base, gram, residual, out):
    count, columns, height, lane = residual.shape
    line = jnp.broadcast_to(jnp.sum(gram[...], axis=0, keepdims=True), (count * count, lane))
    total = jnp.sum(jnp.where(diagonal(count), line, 0.0), axis=1, keepdims=True)
    entry = lambda a, b: total[a * count + b : a * count + b + 1, :]
    lower, inverse = {}, {}
    for a in range(count):
        for b in range(a + 1):
            value = entry(a, b)
            for k in range(b):
                value = value - lower[a, k] * lower[b, k]
            lower[a, b] = jnp.sqrt(value) if a == b else value / lower[b, b]
    for a in range(count):
        inverse[a, a] = 1.0 / lower[a, a]
        for b in range(a):
            value = lower[a, b] * inverse[b, b]
            for k in range(b + 1, a):
                value = value + lower[a, k] * inverse[k, b]
            inverse[a, b] = -value / lower[a, a]
    factors = {at: jnp.broadcast_to(value, (SUB, lane)) for at, value in inverse.items()}
    place = [lax.rem(a + count - base[0], count) for a in range(count)]
    for j in range(columns):
        for at in range(0, height, SUB):
            values = [residual[place[a], j, pl.ds(at, SUB), :] for a in range(count)]
            for a in range(count):
                value = factors[a, 0] * values[0]
                for b in range(1, a + 1):
                    value = value + factors[a, b] * values[b]
                out[a, j, pl.ds(at, SUB), :] = value


def solved(shift, gram, residual):
    return pl.pallas_call(
        solve_kernel,
        out_shape=jax.ShapeDtypeStruct(residual.shape, jnp.float32),
        in_specs=[pl.BlockSpec(memory_space=pltpu.SMEM), VMEM, VMEM],
        out_specs=VMEM,
        compiler_params=pltpu.CompilerParams(vmem_limit_bytes=16 << 20),
        name="solve",
    )(shift, gram, residual)


def from_slab(value, distance):
    size = lax.axis_size("slab")
    return lax.ppermute(value, "slab", [((i + distance) % size, i) for i in range(size)])


def to_next(value, turn=0):
    segs, slabs = lax.axis_size("seg"), lax.axis_size("slab")
    route = []
    for s in range(segs):
        for c in range(slabs):
            route.append((s * slabs + c, (s + 1) % segs * slabs + (c + turn) % slabs))
    return lax.ppermute(value, ("seg", "slab"), route)


def split_vectors(vectors, velocity):
    slabs, mine = lax.axis_size("slab"), lax.axis_index("slab")
    share = vectors.shape[0] // slabs

    def part(distance):
        at = lax.rem(mine + distance, slabs) * share
        return lax.dynamic_slice_in_dim(vectors, at, share, 0)

    start, speeds = [part(0)], [velocity]
    for d in range(1, slabs):
        start.append(from_slab(part(slabs - d), d))
        speeds.append(from_slab(velocity, d))
    firsts = [propagate(speeds, start, i) for i in range(share)]
    previous = [jnp.concatenate([part[i : i + 1] for part in start], 0) for i in range(share)]
    moved, missed = [f[0] for f in firsts], [f[1] for f in firsts]
    for hop in range(1, HOPS):
        for i in range(share):
            message = to_next(moved[i].astype(jnp.float16)).astype(jnp.float32)
            state = (previous[i], message, missed[i])
            if hop + 1 < HOPS:
                previous[i], moved[i], missed[i] = propagate(speeds, state)
            else:
                previous[i], moved[i] = propagate(speeds, state, final=True)
    arrived, begun = [], []
    for d in range(slabs):
        for i in range(share):
            at = (slabs - d) % slabs
            arrived.append(to_next(moved[i][at], at))
            begun.append(from_slab(previous[i][at], d) if d else previous[i][0])
    shift = jnp.full((1,), mine * share, jnp.int32)
    return shift, arrived, begun


def split_rows(vectors, velocity):
    depth, height = velocity.shape[0], vectors.shape[2]

    def pieces(value):
        after = value[..., :depth, :]
        before = value[..., height - depth :, :]
        return [value, from_slab(after, 1), from_slab(before, -1)]

    speeds = pieces(velocity)
    begun = vectors
    for hop in range(HOPS):
        state = pieces(begun)
        arrived = [to_next(propagate_rows(speeds, state, i)) for i in range(vectors.shape[0])]
        if hop + 1 < HOPS:
            begun = jnp.concatenate(arrived, 0) - begun
    return jnp.zeros((1,), jnp.int32), arrived, [begun[i : i + 1] for i in range(vectors.shape[0])]


def shards(block, base_velocity):
    vectors, velocity = tiled(block[0]), tiled(base_velocity[0])
    even = vectors.shape[0] % lax.axis_size("slab") == 0
    shift, arrived, begun = (split_vectors if even else split_rows)(vectors, velocity)
    axes = ("seg", "slab")
    residual, gram = local_gram(shift, arrived, begun, lax.axis_size("seg") * lax.axis_size("slab"))
    gram = lax.all_to_all(gram, axes, 0, 0, tiled=True)
    return untiled(solved(shift, gram, residual))[None]


def solution(mesh):
    placed = (P("seg", None, "slab", None), P("seg", None, None, "slab", None))
    return jax.shard_map(
        shards, mesh=mesh, in_specs=placed, out_specs=P("seg", None, "slab", None), check_vma=False
    )
```

```python
import functools

import jax
import jax.numpy as jnp
from jax import lax
from jax.experimental import pallas as pl
from jax.experimental.pallas import tpu as pltpu
from jax.sharding import PartitionSpec as P

HOPS = 4
SUB = 8
LANE = 128
VMEM = pl.BlockSpec(memory_space=pltpu.VMEM)


def tiled(rows):
    lead, (height, width) = rows.shape[:-2], rows.shape[-2:]
    cut = rows.reshape(lead + (height, width // LANE, LANE))
    return jnp.swapaxes(cut, -3, -2)


def untiled(tiles):
    lead, (count, height, lane) = tiles.shape[:-3], tiles.shape[-3:]
    return jnp.swapaxes(tiles, -3, -2).reshape(lead + (height, count * lane))


def advance(velocity, ping, pong, pieces):
    depth, _, columns, height, _ = velocity[0].shape
    rows = pieces * height
    lane = lax.broadcasted_iota(jnp.int32, (SUB, LANE), 1)
    first, last = lane == 0, lane == LANE - 1

    def step(k, source, target):
        for b in range(rows // SUB):
            piece, at = divmod(SUB * b, height)
            rows_at = pl.ds(SUB + SUB * b, SUB)
            here = [source[j % columns, rows_at, :] for j in (-1, 0, 1)]
            for j in range(columns):
                left, centre, right = here
                west = pltpu.roll(jnp.where(last, left, centre), 1, 1)
                east = pltpu.roll(jnp.where(first, right, centre), LANE - 1, 1)
                up = source[j, pl.ds(SUB + 1 + SUB * b, SUB), :]
                down = source[j, pl.ds(SUB - 1 + SUB * b, SUB), :]
                speed_x = velocity[piece][k, 0, j, pl.ds(at, SUB), :].astype(jnp.float32)
                speed_y = velocity[piece][k, 1, j, pl.ds(at, SUB), :].astype(jnp.float32)
                carried = speed_x * (west - east) + speed_y * (down - up)
                place(target, rows, j, b, 0.9 * centre + ((west + east) + (up + down)) + 0.25 * carried)
                here = [centre, right, source[(j + 2) % columns, rows_at, :]]

    def pair(i, carry):
        step(2 * i, ping, pong)
        step(2 * i + 1, pong, ping)
        return carry

    lax.fori_loop(0, depth // 2, pair, 0)
    if depth % 2:
        step(depth - 1, ping, pong)
        return pong
    return ping


def place(ref, rows, j, b, value):
    ref[j, pl.ds(SUB + SUB * b, SUB), :] = value
    if b == 0:
        ref[j, pl.ds(SUB + rows, 1), :] = value[:1]
    if b == rows // SUB - 1:
        ref[j, pl.ds(SUB - 1, 1), :] = value[SUB - 1 :]


def tiles_of(pieces, columns, height):
    for j in range(columns):
        for b in range(pieces * height // SUB):
            piece, at = divmod(SUB * b, height)
            yield piece, j, pl.ds(at, SUB), b, (piece * columns + j) * (height // SUB) + at // SUB


TOP = 13.0


def propagate_kernel(pieces, index, first, final, *refs):
    refs = list(refs)
    take = lambda count: [refs.pop(0) for _ in range(count)]
    velocity = take(pieces)
    depth, _, columns, height, _ = velocity[0].shape
    rows, count = pieces * height, pieces * columns * height // SUB
    if first:
        previous = take(pieces)
    else:
        previous, message, missed = take(3)
        start = take(pieces) if final else take(1)
    sent = take(pieces) if final else take(1)
    error = None if final else take(1)[0]
    ping, pong = refs
    each = count // len(sent)

    if not first:
        back = jnp.exp2(message[count] - TOP)
    for piece, j, at, b, m in tiles_of(pieces, columns, height):
        if first:
            value = previous[piece][index, j, at, :]
        else:
            value = message[m] * back - previous[piece, j, at, :]
            if final:
                start[piece][0, j, at, :] = value
            else:
                start[0][piece, j, at, :] = value
        place(ping, rows, j, b, value)

    done = advance(velocity, ping, pong, pieces)
    largest = None
    for piece, j, at, b, m in tiles_of(pieces, columns, height):
        value = 0.2**depth * done[j, pl.ds(SUB + SUB * b, SUB), :]
        if not first:
            value = value + missed[m]
        sent[m // each][m % each] = value
        size = jnp.abs(value)
        largest = size if largest is None else jnp.maximum(largest, size)
    largest = jnp.broadcast_to(jnp.max(largest, axis=(0, 1), keepdims=True), (SUB, LANE))
    power = jnp.clip(jnp.floor(jnp.log2(largest)), -100.0, 100.0)
    scale, back = jnp.exp2(TOP - power), jnp.exp2(power - TOP)
    for message in sent:
        message[each] = power
    for m in range(count):
        value = sent[m // each][m % each]
        scaled = value * scale
        wide = scaled * 8193.0
        short = wide - (wide - scaled)
        sent[m // each][m % each] = short
        if not final:
            error[m] = short * back - value


@functools.partial(jax.jit, static_argnames=("index", "final"))
def propagate(velocity, state, index=0, final=False):
    pieces = len(velocity)
    _, _, columns, height, lane = velocity[0].shape
    count = pieces * columns * height // SUB
    first = isinstance(state, list)
    shape = lambda *s: jax.ShapeDtypeStruct(s + (lane,), jnp.float32)
    if final:
        outs = [shape(1, columns, height)] * pieces + [shape(count // pieces + 1, SUB)] * pieces
    else:
        outs = ([] if first else [shape(pieces, columns, height)]) + [shape(count + 1, SUB), shape(count, SUB)]
    scratch = pltpu.VMEM((columns, pieces * height + 2 * SUB, lane), jnp.float32)
    args = [*velocity, *state]
    out = pl.pallas_call(
        functools.partial(propagate_kernel, pieces, index, first, final),
        out_shape=outs,
        in_specs=[VMEM] * len(args),
        out_specs=[VMEM] * len(outs),
        scratch_shapes=[scratch, scratch],
        compiler_params=pltpu.CompilerParams(vmem_limit_bytes=16 << 20),
        name="propagate",
    )(*args)
    return (out[:pieces], out[pieces:]) if final else out


def rows_kernel(pieces, index, *refs):
    velocity, previous, (moved, ping, pong) = refs[:pieces], refs[pieces : 2 * pieces], refs[2 * pieces :]
    depth, _, columns, height, _ = velocity[0].shape
    for piece, j, at, b, _ in tiles_of(pieces, columns, height):
        place(ping, pieces * height, j, b, previous[piece][index, j, at, :])
    done = advance(velocity, ping, pong, pieces)
    for piece, j, at, b, _ in tiles_of(1, columns, height):
        moved[0, j, at, :] = 0.2**depth * done[j, pl.ds(SUB + SUB * b, SUB), :]


@functools.partial(jax.jit, static_argnames=("index",))
def propagate_rows(velocity, state, index):
    pieces = len(velocity)
    _, _, columns, height, lane = velocity[0].shape
    scratch = pltpu.VMEM((columns, pieces * height + 2 * SUB, lane), jnp.float32)
    return pl.pallas_call(
        functools.partial(rows_kernel, pieces, index),
        out_shape=jax.ShapeDtypeStruct((1, columns, height, lane), jnp.float32),
        in_specs=[VMEM] * (2 * pieces),
        out_specs=VMEM,
        scratch_shapes=[scratch, scratch],
        compiler_params=pltpu.CompilerParams(vmem_limit_bytes=16 << 20),
        name="propagate_rows",
    )(*velocity, *state)


def gram_kernel(groups, *refs):
    base, refs = refs[0], refs[1:]
    arrived, start = refs[:groups], refs[groups : 2 * groups]
    residual, gram, lines = refs[2 * groups :]
    count, columns, height, _ = residual.shape
    sums = {}
    coded = len(arrived[0].shape) == 3
    backs = [jnp.exp2(a[a.shape[0] - 1] - TOP) for a in arrived] if coded else []
    for j in range(columns):
        for at in range(0, height, SUB):
            values = [-s[0, j, pl.ds(at, SUB), :] for s in start]
            for p, a in enumerate(arrived):
                if coded:
                    values[p] = a[(j * height + at) // SUB] * backs[p] + values[p]
                else:
                    values[p] = a[0, j, pl.ds(at, SUB), :] + values[p]
            for p in range(count):
                residual[p, j, pl.ds(at, SUB), :] = values[p]
                for q in range(p + 1):
                    term = values[p] * values[q]
                    sums[p, q] = term if (p, q) not in sums else sums[p, q] + term
    for (p, q), total in sums.items():
        line = jnp.sum(total, axis=0, keepdims=True)
        a, b = lax.rem(base[0] + p, count), lax.rem(base[0] + q, count)
        lines[pl.ds(a * count + b, 1), :] = line
        if p != q:
            lines[pl.ds(b * count + a, 1), :] = line
    totals = jnp.where(diagonal(count), jnp.sum(lines[...], axis=1, keepdims=True), 0.0)
    gram[...] = jnp.broadcast_to(jnp.sum(totals, axis=0, keepdims=True), gram.shape)


def diagonal(count):
    shape = (count * count, LANE)
    return lax.broadcasted_iota(jnp.int32, shape, 0) == lax.broadcasted_iota(jnp.int32, shape, 1)


def local_gram(shift, arrived, start, copies):
    count = len(arrived)
    shape = (count,) + start[0].shape[1:]
    return pl.pallas_call(
        functools.partial(gram_kernel, len(arrived)),
        out_shape=[jax.ShapeDtypeStruct(shape, jnp.float32), jax.ShapeDtypeStruct((copies, LANE), jnp.float32)],
        in_specs=[pl.BlockSpec(memory_space=pltpu.SMEM)] + [VMEM] * (2 * len(arrived)),
        out_specs=[VMEM, VMEM],
        scratch_shapes=[pltpu.VMEM((count * count, LANE), jnp.float32)],
        compiler_params=pltpu.CompilerParams(vmem_limit_bytes=16 << 20),
        name="gram",
    )(shift, *arrived, *start)


def solve_kernel(base, gram, residual, out):
    count, columns, height, lane = residual.shape
    line = jnp.broadcast_to(jnp.sum(gram[...], axis=0, keepdims=True), (count * count, lane))
    total = jnp.sum(jnp.where(diagonal(count), line, 0.0), axis=1, keepdims=True)
    entry = lambda a, b: total[a * count + b : a * count + b + 1, :]
    lower, inverse = {}, {}
    for a in range(count):
        for b in range(a + 1):
            value = entry(a, b)
            for k in range(b):
                value = value - lower[a, k] * lower[b, k]
            lower[a, b] = jnp.sqrt(value) if a == b else value / lower[b, b]
    for a in range(count):
        inverse[a, a] = 1.0 / lower[a, a]
        for b in range(a):
            value = lower[a, b] * inverse[b, b]
            for k in range(b + 1, a):
                value = value + lower[a, k] * inverse[k, b]
            inverse[a, b] = -value / lower[a, a]
    factors = {at: jnp.broadcast_to(value, (SUB, lane)) for at, value in inverse.items()}
    place = [lax.rem(a + count - base[0], count) for a in range(count)]
    for j in range(columns):
        for at in range(0, height, SUB):
            values = [residual[place[a], j, pl.ds(at, SUB), :] for a in range(count)]
            for a in range(count):
                value = factors[a, 0] * values[0]
                for b in range(1, a + 1):
                    value = value + factors[a, b] * values[b]
                out[a, j, pl.ds(at, SUB), :] = value


def solved(shift, gram, residual):
    return pl.pallas_call(
        solve_kernel,
        out_shape=jax.ShapeDtypeStruct(residual.shape, jnp.float32),
        in_specs=[pl.BlockSpec(memory_space=pltpu.SMEM), VMEM, VMEM],
        out_specs=VMEM,
        compiler_params=pltpu.CompilerParams(vmem_limit_bytes=16 << 20),
        name="solve",
    )(shift, gram, residual)


def from_slab(value, distance):
    size = lax.axis_size("slab")
    return lax.ppermute(value, "slab", [((i + distance) % size, i) for i in range(size)])


def sent_short(message, turn=0):
    return to_next(message.astype(jnp.float16), turn).astype(jnp.float32)


def to_next(value, turn=0):
    segs, slabs = lax.axis_size("seg"), lax.axis_size("slab")
    route = []
    for s in range(segs):
        for c in range(slabs):
            route.append((s * slabs + c, (s + 1) % segs * slabs + (c + turn) % slabs))
    return lax.ppermute(value, ("seg", "slab"), route)


def split_vectors(vectors, velocity):
    slabs, mine = lax.axis_size("slab"), lax.axis_index("slab")
    share = vectors.shape[0] // slabs

    def part(distance):
        at = lax.rem(mine + distance, slabs) * share
        return lax.dynamic_slice_in_dim(vectors, at, share, 0)

    start, speeds = [part(0)], [velocity]
    for d in range(1, slabs):
        start.append(from_slab(part(slabs - d), d))
        speeds.append(from_slab(velocity, d))
    firsts = [propagate(speeds, start, i) for i in range(share)]
    previous = [jnp.concatenate([part[i : i + 1] for part in start], 0) for i in range(share)]
    moved, missed = [f[0] for f in firsts], [f[1] for f in firsts]
    for hop in range(1, HOPS):
        for i in range(share):
            state = (previous[i], sent_short(moved[i]), missed[i])
            if hop + 1 < HOPS:
                previous[i], moved[i], missed[i] = propagate(speeds, state)
            else:
                previous[i], moved[i] = propagate(speeds, state, final=True)
    arrived, begun = [], []
    for d in range(slabs):
        for i in range(share):
            at = (slabs - d) % slabs
            arrived.append(sent_short(moved[i][at], at))
            begun.append(from_slab(previous[i][at], d) if d else previous[i][0])
    shift = jnp.full((1,), mine * share, jnp.int32)
    return shift, arrived, begun


def split_rows(vectors, velocity):
    depth, height = velocity.shape[0], vectors.shape[2]

    def pieces(value):
        after = value[..., :depth, :]
        before = value[..., height - depth :, :]
        return [value, from_slab(after, 1), from_slab(before, -1)]

    speeds = pieces(velocity)
    begun = vectors
    for hop in range(HOPS):
        state = pieces(begun)
        arrived = [to_next(propagate_rows(speeds, state, i)) for i in range(vectors.shape[0])]
        if hop + 1 < HOPS:
            begun = jnp.concatenate(arrived, 0) - begun
    return jnp.zeros((1,), jnp.int32), arrived, [begun[i : i + 1] for i in range(vectors.shape[0])]


def shards(block, base_velocity):
    vectors, velocity = tiled(block[0]), tiled(base_velocity[0])
    even = vectors.shape[0] % lax.axis_size("slab") == 0
    shift, arrived, begun = (split_vectors if even else split_rows)(vectors, velocity)
    axes = ("seg", "slab")
    residual, gram = local_gram(shift, arrived, begun, lax.axis_size("seg") * lax.axis_size("slab"))
    gram = lax.all_to_all(gram, axes, 0, 0, tiled=True)
    return untiled(solved(shift, gram, residual))[None]


def solution(mesh):
    placed = (P("seg", None, "slab", None), P("seg", None, None, "slab", None))
    return jax.shard_map(
        shards, mesh=mesh, in_specs=placed, out_specs=P("seg", None, "slab", None), check_vma=False
    )
```

```python
import functools

import jax
import jax.numpy as jnp
from jax import lax
from jax.experimental import pallas as pl
from jax.experimental.pallas import tpu as pltpu
from jax.sharding import PartitionSpec as P

HOPS = 4
SUB = 8
LANE = 128
VMEM = pl.BlockSpec(memory_space=pltpu.VMEM)
SMEM = pl.BlockSpec(memory_space=pltpu.SMEM)


def tiled(rows):
    lead, (height, width) = rows.shape[:-2], rows.shape[-2:]
    cut = rows.reshape(lead + (height, width // LANE, LANE))
    return jnp.swapaxes(cut, -3, -2)


def untiled(tiles):
    lead, (count, height, lane) = tiles.shape[:-3], tiles.shape[-3:]
    return jnp.swapaxes(tiles, -3, -2).reshape(lead + (height, count * lane))


def advance(velocity, ping, pong, pieces):
    depth, _, columns, height, _ = velocity[0].shape
    rows = pieces * height
    lane = lax.broadcasted_iota(jnp.int32, (SUB, LANE), 1)
    first, last = lane == 0, lane == LANE - 1

    def step(k, source, target):
        for b in range(rows // SUB):
            piece, at = divmod(SUB * b, height)
            rows_at = pl.ds(SUB + SUB * b, SUB)
            here = [source[j % columns, rows_at, :] for j in (-1, 0, 1)]
            for j in range(columns):
                left, centre, right = here
                west = pltpu.roll(jnp.where(last, left, centre), 1, 1)
                east = pltpu.roll(jnp.where(first, right, centre), LANE - 1, 1)
                up = source[j, pl.ds(SUB + 1 + SUB * b, SUB), :]
                down = source[j, pl.ds(SUB - 1 + SUB * b, SUB), :]
                speed_x = velocity[piece][k, 0, j, pl.ds(at, SUB), :].astype(jnp.float32)
                speed_y = velocity[piece][k, 1, j, pl.ds(at, SUB), :].astype(jnp.float32)
                carried = speed_x * (west - east) + speed_y * (down - up)
                place(target, rows, j, b, 0.9 * centre + ((west + east) + (up + down)) + 0.25 * carried)
                here = [centre, right, source[(j + 2) % columns, rows_at, :]]

    def pair(i, carry):
        step(2 * i, ping, pong)
        step(2 * i + 1, pong, ping)
        return carry

    lax.fori_loop(0, depth // 2, pair, 0)
    if depth % 2:
        step(depth - 1, ping, pong)
        return pong
    return ping


def place(ref, rows, j, b, value):
    ref[j, pl.ds(SUB + SUB * b, SUB), :] = value
    if b == 0:
        ref[j, pl.ds(SUB + rows, 1), :] = value[:1]
    if b == rows // SUB - 1:
        ref[j, pl.ds(SUB - 1, 1), :] = value[SUB - 1 :]


def tiles_of(pieces, columns, height):
    for j in range(columns):
        for b in range(pieces * height // SUB):
            piece, at = divmod(SUB * b, height)
            yield piece, j, pl.ds(at, SUB), b, (piece * columns + j) * (height // SUB) + at // SUB


TOP = 13.0


def take_in(cases, use):
    def run(message, previous):
        count = message.shape[0] - 1
        back = jnp.exp2(message[count] - TOP)
        pieces, columns, height, _ = previous.shape
        for piece, j, at, b, m in tiles_of(pieces, columns, height):
            use(piece, j, at, b, message[m] * back - previous[piece, j, at, :])

    for chosen, message, previous in cases:
        pl.when(chosen)(functools.partial(run, message, previous))


def propagate_kernel(pieces, index, first, last, *refs):
    refs = list(refs)
    take = lambda count: [refs.pop(0) for _ in range(count)]
    (flags,) = take(1)
    velocity = take(pieces)
    depth, _, columns, height, _ = velocity[0].shape
    rows, count = pieces * height, pieces * columns * height // SUB
    if first:
        previous = take(pieces)
    else:
        previous, missed, message = take(3)
        wrapped = None if last else take(1)[0]
        (start,) = take(1)
    sent, error, ping, pong = refs

    @pl.when(flags[0] == (1 if last else 0))
    def _():
        def use(piece, j, at, b, value):
            start[piece, j, at, :] = value
            place(ping, rows, j, b, value)

        if first:
            for piece, j, at, b, m in tiles_of(pieces, columns, height):
                place(ping, rows, j, b, previous[piece][index, j, at, :])
        elif last:
            take_in([(flags[0] == 1, message, previous)], use)
        else:
            at_first = flags[1] == 1
            take_in([(at_first, wrapped, previous), (jnp.logical_not(at_first), message, previous)], use)

        done = advance(velocity, ping, pong, pieces)
        largest = None
        for piece, j, at, b, m in tiles_of(pieces, columns, height):
            value = 0.2**depth * done[j, pl.ds(SUB + SUB * b, SUB), :]
            if not first:
                value = value + missed[m]
            sent[m] = value
            size = jnp.abs(value)
            largest = size if largest is None else jnp.maximum(largest, size)
        largest = jnp.broadcast_to(jnp.max(largest, axis=(0, 1), keepdims=True), (SUB, LANE))
        power = jnp.clip(jnp.floor(jnp.log2(largest)), -100.0, 100.0)
        scale, back = jnp.exp2(TOP - power), jnp.exp2(power - TOP)
        sent[count] = power
        for m in range(count):
            value = sent[m]
            scaled = value * scale
            wide = scaled * 8193.0
            short = wide - (wide - scaled)
            sent[m] = short
            error[m] = short * back - value


@functools.partial(jax.jit, static_argnames=("index", "last"))
def propagate(flags, velocity, state, index=0, last=False):
    pieces = len(velocity)
    _, _, columns, height, lane = velocity[0].shape
    count = pieces * columns * height // SUB
    first = isinstance(state, list)
    shape = lambda *s: jax.ShapeDtypeStruct(s + (lane,), jnp.float32)
    outs = ([] if first else [shape(pieces, columns, height)]) + [shape(count + 1, SUB), shape(count, SUB)]
    scratch = pltpu.VMEM((columns, pieces * height + 2 * SUB, lane), jnp.float32)
    args = [*velocity, *state]
    return pl.pallas_call(
        functools.partial(propagate_kernel, pieces, index, first, last),
        out_shape=outs,
        in_specs=[SMEM] + [VMEM] * len(args),
        out_specs=[VMEM] * len(outs),
        scratch_shapes=[scratch, scratch],
        compiler_params=pltpu.CompilerParams(vmem_limit_bytes=16 << 20),
        name="propagate_last" if last else "propagate",
    )(flags, *args)


def residual_kernel(flags, message, wrapped, previous, previous_last, *outs):
    def use(piece, j, at, b, value):
        outs[piece][0, j, at, :] = value

    at_last, at_first = flags[0] == 1, flags[1] == 1
    rest = jnp.logical_not(jnp.logical_or(at_last, at_first))
    cases = [(at_last, message, previous_last), (at_first, wrapped, previous), (rest, message, previous)]
    take_in(cases, use)


@jax.jit
def last_residual(flags, *state):
    pieces, columns, height, lane = state[2].shape
    return pl.pallas_call(
        residual_kernel,
        out_shape=[jax.ShapeDtypeStruct((1, columns, height, lane), jnp.float32)] * pieces,
        in_specs=[SMEM] + [VMEM] * len(state),
        out_specs=[VMEM] * pieces,
        compiler_params=pltpu.CompilerParams(vmem_limit_bytes=16 << 20),
        name="residual",
    )(flags, *state)


def rows_kernel(pieces, index, *refs):
    velocity, previous, (moved, ping, pong) = refs[:pieces], refs[pieces : 2 * pieces], refs[2 * pieces :]
    depth, _, columns, height, _ = velocity[0].shape
    for piece, j, at, b, _ in tiles_of(pieces, columns, height):
        place(ping, pieces * height, j, b, previous[piece][index, j, at, :])
    done = advance(velocity, ping, pong, pieces)
    for piece, j, at, b, _ in tiles_of(1, columns, height):
        moved[0, j, at, :] = 0.2**depth * done[j, pl.ds(SUB + SUB * b, SUB), :]


@functools.partial(jax.jit, static_argnames=("index",))
def propagate_rows(velocity, state, index):
    pieces = len(velocity)
    _, _, columns, height, lane = velocity[0].shape
    scratch = pltpu.VMEM((columns, pieces * height + 2 * SUB, lane), jnp.float32)
    return pl.pallas_call(
        functools.partial(rows_kernel, pieces, index),
        out_shape=jax.ShapeDtypeStruct((1, columns, height, lane), jnp.float32),
        in_specs=[VMEM] * (2 * pieces),
        out_specs=VMEM,
        scratch_shapes=[scratch, scratch],
        compiler_params=pltpu.CompilerParams(vmem_limit_bytes=16 << 20),
        name="propagate_rows",
    )(*velocity, *state)


def gram_kernel(base, *refs):
    residual, (gram, lines) = refs[:-2], refs[-2:]
    count = len(residual)
    _, columns, height, _ = residual[0].shape
    sums = {}
    for j in range(columns):
        for at in range(0, height, SUB):
            values = [r[0, j, pl.ds(at, SUB), :] for r in residual]
            for p in range(count):
                for q in range(p + 1):
                    term = values[p] * values[q]
                    sums[p, q] = term if (p, q) not in sums else sums[p, q] + term
    for (p, q), total in sums.items():
        line = jnp.sum(total, axis=0, keepdims=True)
        a, b = lax.rem(base[0] + p, count), lax.rem(base[0] + q, count)
        lines[pl.ds(a * count + b, 1), :] = line
        if p != q:
            lines[pl.ds(b * count + a, 1), :] = line
    totals = jnp.where(diagonal(count), jnp.sum(lines[...], axis=1, keepdims=True), 0.0)
    gram[...] = jnp.broadcast_to(jnp.sum(totals, axis=0, keepdims=True), gram.shape)


def diagonal(count):
    shape = (count * count, LANE)
    return lax.broadcasted_iota(jnp.int32, shape, 0) == lax.broadcasted_iota(jnp.int32, shape, 1)


def local_gram(shift, residual, copies):
    count = len(residual)
    return pl.pallas_call(
        gram_kernel,
        out_shape=jax.ShapeDtypeStruct((copies, LANE), jnp.float32),
        in_specs=[SMEM] + [VMEM] * count,
        out_specs=VMEM,
        scratch_shapes=[pltpu.VMEM((count * count, LANE), jnp.float32)],
        compiler_params=pltpu.CompilerParams(vmem_limit_bytes=16 << 20),
        name="gram",
    )(shift, *residual)


def solve_kernel(base, gram, *refs):
    residual, out = refs[:-1], refs[-1]
    count, columns, height, lane = out.shape
    line = jnp.broadcast_to(jnp.sum(gram[...], axis=0, keepdims=True), (count * count, lane))
    total = jnp.sum(jnp.where(diagonal(count), line, 0.0), axis=1, keepdims=True)
    entry = lambda a, b: total[a * count + b : a * count + b + 1, :]
    lower, inverse = {}, {}
    for a in range(count):
        for b in range(a + 1):
            value = entry(a, b)
            for k in range(b):
                value = value - lower[a, k] * lower[b, k]
            lower[a, b] = jnp.sqrt(value) if a == b else value / lower[b, b]
    for a in range(count):
        inverse[a, a] = 1.0 / lower[a, a]
        for b in range(a):
            value = lower[a, b] * inverse[b, b]
            for k in range(b + 1, a):
                value = value + lower[a, k] * inverse[k, b]
            inverse[a, b] = -value / lower[a, a]
    factors = {at: jnp.broadcast_to(value, (SUB, lane)) for at, value in inverse.items()}

    def finish(place):
        for j in range(columns):
            for at in range(0, height, SUB):
                values = [residual[place[a]][0, j, pl.ds(at, SUB), :] for a in range(count)]
                for a in range(count):
                    value = factors[a, 0] * values[0]
                    for b in range(1, a + 1):
                        value = value + factors[a, b] * values[b]
                    out[a, j, pl.ds(at, SUB), :] = value

    for turn in range(count):
        pl.when(base[0] == turn)(functools.partial(finish, [(a - turn) % count for a in range(count)]))


def solved(shift, gram, residual):
    count, (_, columns, height, lane) = len(residual), residual[0].shape
    return pl.pallas_call(
        solve_kernel,
        out_shape=jax.ShapeDtypeStruct((count, columns, height, lane), jnp.float32),
        in_specs=[SMEM, VMEM] + [VMEM] * count,
        out_specs=VMEM,
        compiler_params=pltpu.CompilerParams(vmem_limit_bytes=16 << 20),
        name="solve",
    )(shift, gram, *residual)


def from_slab(value, distance):
    size = lax.axis_size("slab")
    return lax.ppermute(value, "slab", [((i + distance) % size, i) for i in range(size)])


def to_next(value, segments=None):
    size = lax.axis_size("seg")
    return lax.ppermute(value, "seg", [(i, (i + 1) % size) for i in segments or range(size)])


def sent_short(message, segments=None):
    return to_next(message.astype(jnp.float16), segments).astype(jnp.float32)


def split_vectors(vectors, velocity):
    slabs, mine = lax.axis_size("slab"), lax.axis_index("slab")
    share = vectors.shape[0] // slabs

    def part(distance):
        at = lax.rem(mine + distance, slabs) * share
        return lax.dynamic_slice_in_dim(vectors, at, share, 0)

    start, speeds = [part(0)], [velocity]
    for d in range(1, slabs):
        start.append(from_slab(part(slabs - d), d))
        speeds.append(from_slab(velocity, d))
    here, end = lax.axis_index("seg"), lax.axis_size("seg") - 1
    flags = jnp.stack([here == end, here == 0]).astype(jnp.int32)
    previous = [jnp.concatenate([part[i : i + 1] for part in start], 0) for i in range(share)]
    own, ends = list(previous), list(previous)
    arrived, wrapped, missed, missed_end = [[None] * share for _ in range(4)]
    for hop in range(HOPS):
        for i in range(share):
            if hop == 0:
                sent_end, missed_end[i] = propagate(flags, speeds, start, i, last=True)
                sent, missed[i] = propagate(flags, speeds, start, i)
            else:
                state = (ends[i], missed_end[i], arrived[i])
                ends[i], sent_end, missed_end[i] = propagate(flags, speeds, state, last=True)
                state = (own[i], missed[i], arrived[i], wrapped[i])
                own[i], sent, missed[i] = propagate(flags, speeds, state)
            wrapped[i] = sent_short(sent_end, [end])
            arrived[i] = sent_short(sent)
    parts = [last_residual(flags, arrived[i], wrapped[i], own[i], ends[i]) for i in range(share)]
    residual = []
    for d in range(slabs):
        for i in range(share):
            part_i = parts[i][(slabs - d) % slabs]
            residual.append(from_slab(part_i, d) if d else part_i)
    return jnp.full((1,), mine * share, jnp.int32), residual


def split_rows(vectors, velocity):
    depth, height = velocity.shape[0], vectors.shape[2]

    def pieces(value):
        after = value[..., :depth, :]
        before = value[..., height - depth :, :]
        return [value, from_slab(after, 1), from_slab(before, -1)]

    speeds = pieces(velocity)
    begun = vectors
    for hop in range(HOPS):
        state = pieces(begun)
        arrived = [to_next(propagate_rows(speeds, state, i)) for i in range(vectors.shape[0])]
        begun = jnp.concatenate(arrived, 0) - begun
    return jnp.zeros((1,), jnp.int32), [begun[i : i + 1] for i in range(vectors.shape[0])]


def shards(block, base_velocity):
    vectors, velocity = tiled(block[0]), tiled(base_velocity[0])
    even = vectors.shape[0] % lax.axis_size("slab") == 0
    shift, residual = (split_vectors if even else split_rows)(vectors, velocity)
    axes = ("seg", "slab")
    gram = local_gram(shift, residual, lax.axis_size("seg") * lax.axis_size("slab"))
    gram = lax.all_to_all(gram, axes, 0, 0, tiled=True)
    return untiled(solved(shift, gram, residual))[None]


def solution(mesh):
    placed = (P("seg", None, "slab", None), P("seg", None, None, "slab", None))
    return jax.shard_map(
        shards, mesh=mesh, in_specs=placed, out_specs=P("seg", None, "slab", None), check_vma=False
    )
```

```python
import functools

import jax
import jax.numpy as jnp
from jax import lax
from jax.experimental import pallas as pl
from jax.experimental.pallas import tpu as pltpu
from jax.sharding import PartitionSpec as P


HOPS = 4
SUB = 8
LANE = 128
VMEM = pl.BlockSpec(memory_space=pltpu.VMEM)
SMEM = pl.BlockSpec(memory_space=pltpu.SMEM)


def tiled(rows):
    lead, (height, width) = rows.shape[:-2], rows.shape[-2:]
    cut = rows.reshape(lead + (height, width // LANE, LANE))
    return jnp.swapaxes(cut, -3, -2)


def untiled(tiles):
    lead, (count, height, lane) = tiles.shape[:-3], tiles.shape[-3:]
    return jnp.swapaxes(tiles, -3, -2).reshape(lead + (height, count * lane))


def advance(velocity, ping, pong, pieces):
    depth, _, columns, height, _ = velocity[0].shape
    rows = pieces * height
    lane = lax.broadcasted_iota(jnp.int32, (SUB, LANE), 1)
    first, last = lane == 0, lane == LANE - 1

    def step(k, source, target):
        for b in range(rows // SUB):
            piece, at = divmod(SUB * b, height)
            rows_at = pl.ds(SUB + SUB * b, SUB)
            here = [source[j % columns, rows_at, :] for j in (-1, 0, 1)]
            for j in range(columns):
                left, centre, right = here
                west = pltpu.roll(jnp.where(last, left, centre), 1, 1)
                east = pltpu.roll(jnp.where(first, right, centre), LANE - 1, 1)
                up = source[j, pl.ds(SUB + 1 + SUB * b, SUB), :]
                down = source[j, pl.ds(SUB - 1 + SUB * b, SUB), :]
                speed_x = velocity[piece][k, 0, j, pl.ds(at, SUB), :].astype(jnp.float32)
                speed_y = velocity[piece][k, 1, j, pl.ds(at, SUB), :].astype(jnp.float32)
                carried = speed_x * (west - east) + speed_y * (down - up)
                place(target, rows, j, b, 0.9 * centre + ((west + east) + (up + down)) + 0.25 * carried)
                here = [centre, right, source[(j + 2) % columns, rows_at, :]]

    def pair(i, carry):
        step(2 * i, ping, pong)
        step(2 * i + 1, pong, ping)
        return carry

    lax.fori_loop(0, depth // 2, pair, 0)
    if depth % 2:
        step(depth - 1, ping, pong)
        return pong
    return ping


def place(ref, rows, j, b, value):
    ref[j, pl.ds(SUB + SUB * b, SUB), :] = value
    if b == 0:
        ref[j, pl.ds(SUB + rows, 1), :] = value[:1]
    if b == rows // SUB - 1:
        ref[j, pl.ds(SUB - 1, 1), :] = value[SUB - 1 :]


def tiles_of(pieces, columns, height):
    for j in range(columns):
        for b in range(pieces * height // SUB):
            piece, at = divmod(SUB * b, height)
            yield piece, j, pl.ds(at, SUB), b, (piece * columns + j) * (height // SUB) + at // SUB


TOP = 13.0


def take_in(cases, use):
    def run(message, previous):
        count = message.shape[0] - 1
        back = jnp.exp2(message[count] - TOP)
        pieces, columns, height, _ = previous.shape
        for piece, j, at, b, m in tiles_of(pieces, columns, height):
            use(piece, j, at, b, message[m] * back - previous[piece, j, at, :])

    for chosen, message, previous in cases:
        pl.when(chosen)(functools.partial(run, message, previous))


def propagate_kernel(pieces, index, first, last, *refs):
    refs = list(refs)
    take = lambda count: [refs.pop(0) for _ in range(count)]
    (flags,) = take(1)
    velocity = take(pieces)
    depth, _, columns, height, _ = velocity[0].shape
    rows, count = pieces * height, pieces * columns * height // SUB
    if first:
        previous = take(pieces)
    else:
        previous, missed, message = take(3)
        wrapped = None if last else take(1)[0]
        (start,) = take(1)
    sent, error, ping, pong = refs

    @pl.when(flags[0] == (1 if last else 0))
    def _():
        def use(piece, j, at, b, value):
            start[piece, j, at, :] = value
            place(ping, rows, j, b, value)

        if first:
            for piece, j, at, b, m in tiles_of(pieces, columns, height):
                place(ping, rows, j, b, previous[piece][index, j, at, :])
        elif last:
            take_in([(flags[0] == 1, message, previous)], use)
        else:
            at_first = flags[1] == 1
            take_in([(at_first, wrapped, previous), (jnp.logical_not(at_first), message, previous)], use)

        done = advance(velocity, ping, pong, pieces)
        largest = None
        for piece, j, at, b, m in tiles_of(pieces, columns, height):
            value = 0.2**depth * done[j, pl.ds(SUB + SUB * b, SUB), :]
            if not first:
                value = value + missed[m]
            sent[m] = value
            size = jnp.abs(value)
            largest = size if largest is None else jnp.maximum(largest, size)
        largest = jnp.broadcast_to(jnp.max(largest, axis=(0, 1), keepdims=True), (SUB, LANE))
        power = jnp.clip(jnp.floor(jnp.log2(largest)), -100.0, 100.0)
        scale, back = jnp.exp2(TOP - power), jnp.exp2(power - TOP)
        sent[count] = power
        for m in range(count):
            value = sent[m]
            scaled = value * scale
            wide = scaled * 8193.0
            short = wide - (wide - scaled)
            sent[m] = short
            error[m] = short * back - value


@functools.partial(jax.jit, static_argnames=("index", "last"))
def propagate(flags, velocity, state, index=0, last=False):
    pieces = len(velocity)
    _, _, columns, height, lane = velocity[0].shape
    count = pieces * columns * height // SUB
    first = isinstance(state, list)
    shape = lambda *s: jax.ShapeDtypeStruct(s + (lane,), jnp.float32)
    outs = ([] if first else [shape(pieces, columns, height)]) + [shape(count + 1, SUB), shape(count, SUB)]
    scratch = pltpu.VMEM((columns, pieces * height + 2 * SUB, lane), jnp.float32)
    args = [*velocity, *state]
    return pl.pallas_call(
        functools.partial(propagate_kernel, pieces, index, first, last),
        out_shape=outs,
        in_specs=[SMEM] + [VMEM] * len(args),
        out_specs=[VMEM] * len(outs),
        scratch_shapes=[scratch, scratch],
        compiler_params=pltpu.CompilerParams(vmem_limit_bytes=16 << 20),
        name="propagate_last" if last else "propagate",
    )(flags, *args)


def residual_kernel(flags, message, wrapped, previous, previous_last, *outs):
    def use(piece, j, at, b, value):
        outs[piece][0, j, at, :] = value

    at_last, at_first = flags[0] == 1, flags[1] == 1
    rest = jnp.logical_not(jnp.logical_or(at_last, at_first))
    cases = [(at_last, message, previous_last), (at_first, wrapped, previous), (rest, message, previous)]
    take_in(cases, use)


@jax.jit
def last_residual(flags, *state):
    pieces, columns, height, lane = state[2].shape
    return pl.pallas_call(
        residual_kernel,
        out_shape=[jax.ShapeDtypeStruct((1, columns, height, lane), jnp.float32)] * pieces,
        in_specs=[SMEM] + [VMEM] * len(state),
        out_specs=[VMEM] * pieces,
        compiler_params=pltpu.CompilerParams(vmem_limit_bytes=16 << 20),
        name="residual",
    )(flags, *state)


def rows_kernel(pieces, index, *refs):
    velocity, previous, (moved, ping, pong) = refs[:pieces], refs[pieces : 2 * pieces], refs[2 * pieces :]
    depth, _, columns, height, _ = velocity[0].shape
    for piece, j, at, b, _ in tiles_of(pieces, columns, height):
        place(ping, pieces * height, j, b, previous[piece][index, j, at, :])
    done = advance(velocity, ping, pong, pieces)
    for piece, j, at, b, _ in tiles_of(1, columns, height):
        moved[0, j, at, :] = 0.2**depth * done[j, pl.ds(SUB + SUB * b, SUB), :]


@functools.partial(jax.jit, static_argnames=("index",))
def propagate_rows(velocity, state, index):
    pieces = len(velocity)
    _, _, columns, height, lane = velocity[0].shape
    scratch = pltpu.VMEM((columns, pieces * height + 2 * SUB, lane), jnp.float32)
    return pl.pallas_call(
        functools.partial(rows_kernel, pieces, index),
        out_shape=jax.ShapeDtypeStruct((1, columns, height, lane), jnp.float32),
        in_specs=[VMEM] * (2 * pieces),
        out_specs=VMEM,
        scratch_shapes=[scratch, scratch],
        compiler_params=pltpu.CompilerParams(vmem_limit_bytes=16 << 20),
        name="propagate_rows",
    )(*velocity, *state)


def gram_kernel(base, *refs):
    residual, (gram, lines) = refs[:-2], refs[-2:]
    count = len(residual)
    _, columns, height, _ = residual[0].shape
    sums = {}
    for j in range(columns):
        for at in range(0, height, SUB):
            values = [r[0, j, pl.ds(at, SUB), :] for r in residual]
            for p in range(count):
                for q in range(p + 1):
                    term = values[p] * values[q]
                    sums[p, q] = term if (p, q) not in sums else sums[p, q] + term
    for (p, q), total in sums.items():
        line = jnp.sum(total, axis=0, keepdims=True)
        a, b = lax.rem(base[0] + p, count), lax.rem(base[0] + q, count)
        lines[pl.ds(a * count + b, 1), :] = line
        if p != q:
            lines[pl.ds(b * count + a, 1), :] = line
    totals = jnp.where(diagonal(count), jnp.sum(lines[...], axis=1, keepdims=True), 0.0)
    gram[...] = jnp.broadcast_to(jnp.sum(totals, axis=0, keepdims=True), gram.shape)


def diagonal(count):
    shape = (count * count, LANE)
    return lax.broadcasted_iota(jnp.int32, shape, 0) == lax.broadcasted_iota(jnp.int32, shape, 1)


def local_gram(shift, residual, copies):
    count = len(residual)
    return pl.pallas_call(
        gram_kernel,
        out_shape=jax.ShapeDtypeStruct((copies, LANE), jnp.float32),
        in_specs=[SMEM] + [VMEM] * count,
        out_specs=VMEM,
        scratch_shapes=[pltpu.VMEM((count * count, LANE), jnp.float32)],
        compiler_params=pltpu.CompilerParams(vmem_limit_bytes=16 << 20),
        name="gram",
    )(shift, *residual)


def solve_kernel(base, gram, *refs):
    residual, out = refs[:-1], refs[-1]
    count, columns, height, lane = out.shape
    line = jnp.broadcast_to(jnp.sum(gram[...], axis=0, keepdims=True), (count * count, lane))
    total = jnp.sum(jnp.where(diagonal(count), line, 0.0), axis=1, keepdims=True)
    entry = lambda a, b: total[a * count + b : a * count + b + 1, :]
    lower, inverse = {}, {}
    for a in range(count):
        for b in range(a + 1):
            value = entry(a, b)
            for k in range(b):
                value = value - lower[a, k] * lower[b, k]
            lower[a, b] = jnp.sqrt(value) if a == b else value / lower[b, b]
    for a in range(count):
        inverse[a, a] = 1.0 / lower[a, a]
        for b in range(a):
            value = lower[a, b] * inverse[b, b]
            for k in range(b + 1, a):
                value = value + lower[a, k] * inverse[k, b]
            inverse[a, b] = -value / lower[a, a]
    factors = {at: jnp.broadcast_to(value, (SUB, lane)) for at, value in inverse.items()}

    def finish(place):
        for j in range(columns):
            for at in range(0, height, SUB):
                values = [residual[place[a]][0, j, pl.ds(at, SUB), :] for a in range(count)]
                for a in range(count):
                    value = factors[a, 0] * values[0]
                    for b in range(1, a + 1):
                        value = value + factors[a, b] * values[b]
                    out[a, j, pl.ds(at, SUB), :] = value

    for turn in range(count):
        pl.when(base[0] == turn)(functools.partial(finish, [(a - turn) % count for a in range(count)]))


def solved(shift, gram, residual):
    count, (_, columns, height, lane) = len(residual), residual[0].shape
    return pl.pallas_call(
        solve_kernel,
        out_shape=jax.ShapeDtypeStruct((count, columns, height, lane), jnp.float32),
        in_specs=[SMEM, VMEM] + [VMEM] * count,
        out_specs=VMEM,
        compiler_params=pltpu.CompilerParams(vmem_limit_bytes=16 << 20),
        name="solve",
    )(shift, gram, *residual)


def from_slab(value, distance):
    size = lax.axis_size("slab")
    return lax.ppermute(value, "slab", [((i + distance) % size, i) for i in range(size)])


def to_next(value, segments=None):
    size = lax.axis_size("seg")
    return lax.ppermute(value, "seg", [(i, (i + 1) % size) for i in segments or range(size)])


def sent_short(message, segments=None):
    return to_next(message.astype(jnp.float16), segments).astype(jnp.float32)


def split_vectors(vectors, velocity):
    slabs, mine = lax.axis_size("slab"), lax.axis_index("slab")
    share = vectors.shape[0] // slabs

    def part(distance):
        at = lax.rem(mine + distance, slabs) * share
        return lax.dynamic_slice_in_dim(vectors, at, share, 0)

    start, speeds = [part(0)], [velocity]
    for d in range(1, slabs):
        start.append(from_slab(part(slabs - d), d))
        speeds.append(from_slab(velocity, d))
    here, end = lax.axis_index("seg"), lax.axis_size("seg") - 1
    flags = jnp.stack([here == end, here == 0]).astype(jnp.int32)
    previous = [jnp.concatenate([part[i : i + 1] for part in start], 0) for i in range(share)]
    own, ends = list(previous), list(previous)
    arrived, wrapped, missed, missed_end = [[None] * share for _ in range(4)]
    for hop in range(HOPS):
        for i in range(share):
            if hop == 0:
                state_end, state = start, start
            else:
                state_end = (ends[i], missed_end[i], arrived[i])
                state = (own[i], missed[i], arrived[i], wrapped[i])
            *began_end, sent_end, missed_end[i] = propagate(flags, speeds, state_end, i if hop == 0 else 0, last=True)
            *began, sent, missed[i] = propagate(flags, speeds, state, i if hop == 0 else 0)
            if hop:
                ends[i], own[i] = began_end[0], began[0]
            wrapped[i] = sent_short(sent_end, [end])
            arrived[i] = sent_short(sent)
    parts = [last_residual(flags, arrived[i], wrapped[i], own[i], ends[i]) for i in range(share)]
    residual = []
    for d in range(slabs):
        for i in range(share):
            part_i = parts[i][(slabs - d) % slabs]
            residual.append(from_slab(part_i, d) if d else part_i)
    return jnp.full((1,), mine * share, jnp.int32), residual


def split_rows(vectors, velocity):
    depth, height = velocity.shape[0], vectors.shape[2]

    def pieces(value):
        after = value[..., :depth, :]
        before = value[..., height - depth :, :]
        return [value, from_slab(after, 1), from_slab(before, -1)]

    speeds = pieces(velocity)
    begun = vectors
    for _ in range(HOPS):
        state = pieces(begun)
        arrived = [to_next(propagate_rows(speeds, state, i)) for i in range(vectors.shape[0])]
        begun = jnp.concatenate(arrived, 0) - begun
    return jnp.zeros((1,), jnp.int32), [begun[i : i + 1] for i in range(vectors.shape[0])]


def shards(block, base_velocity):
    vectors, velocity = tiled(block[0]), tiled(base_velocity[0])
    even = vectors.shape[0] % lax.axis_size("slab") == 0
    shift, residual = (split_vectors if even else split_rows)(vectors, velocity)
    axes = ("seg", "slab")
    gram = local_gram(shift, residual, lax.axis_size("seg") * lax.axis_size("slab"))
    gram = lax.all_to_all(gram, axes, 0, 0, tiled=True)
    return untiled(solved(shift, gram, residual))[None]


def solution(mesh):
    placed = (P("seg", None, "slab", None), P("seg", None, None, "slab", None))
    return jax.shard_map(
        shards, mesh=mesh, in_specs=placed, out_specs=P("seg", None, "slab", None), check_vma=False
    )
```

```python
import functools

import jax
import jax.numpy as jnp
from jax import lax
from jax.experimental import pallas as pl
from jax.experimental.pallas import tpu as pltpu
from jax.sharding import PartitionSpec as P


HOPS = 4
SUB = 8
LANE = 128
VMEM = pl.BlockSpec(memory_space=pltpu.VMEM)


def tiled(rows):
    lead, (height, width) = rows.shape[:-2], rows.shape[-2:]
    cut = rows.reshape(lead + (height, width // LANE, LANE))
    return jnp.swapaxes(cut, -3, -2)


def untiled(tiles):
    lead, (count, height, lane) = tiles.shape[:-3], tiles.shape[-3:]
    return jnp.swapaxes(tiles, -3, -2).reshape(lead + (height, count * lane))


def advance(velocity, ping, pong, pieces):
    depth, _, columns, height, _ = velocity[0].shape
    rows = pieces * height
    lane = lax.broadcasted_iota(jnp.int32, (SUB, LANE), 1)
    first, last = lane == 0, lane == LANE - 1

    def step(k, source, target):
        for b in range(rows // SUB):
            piece, at = divmod(SUB * b, height)
            rows_at = pl.ds(SUB + SUB * b, SUB)
            here = [source[j % columns, rows_at, :] for j in (-1, 0, 1)]
            for j in range(columns):
                left, centre, right = here
                west = pltpu.roll(jnp.where(last, left, centre), 1, 1)
                east = pltpu.roll(jnp.where(first, right, centre), LANE - 1, 1)
                up = source[j, pl.ds(SUB + 1 + SUB * b, SUB), :]
                down = source[j, pl.ds(SUB - 1 + SUB * b, SUB), :]
                speed_x = velocity[piece][k, 0, j, pl.ds(at, SUB), :].astype(jnp.float32)
                speed_y = velocity[piece][k, 1, j, pl.ds(at, SUB), :].astype(jnp.float32)
                carried = speed_x * (west - east) + speed_y * (down - up)
                place(target, rows, j, b, 0.9 * centre + ((west + east) + (up + down)) + 0.25 * carried)
                here = [centre, right, source[(j + 2) % columns, rows_at, :]]

    def pair(i, carry):
        step(2 * i, ping, pong)
        step(2 * i + 1, pong, ping)
        return carry

    lax.fori_loop(0, depth // 2, pair, 0)
    if depth % 2:
        step(depth - 1, ping, pong)
        return pong
    return ping


def place(ref, rows, j, b, value):
    ref[j, pl.ds(SUB + SUB * b, SUB), :] = value
    if b == 0:
        ref[j, pl.ds(SUB + rows, 1), :] = value[:1]
    if b == rows // SUB - 1:
        ref[j, pl.ds(SUB - 1, 1), :] = value[SUB - 1 :]


def tiles_of(pieces, columns, height):
    for j in range(columns):
        for b in range(pieces * height // SUB):
            piece, at = divmod(SUB * b, height)
            yield piece, j, pl.ds(at, SUB), b, (piece * columns + j) * (height // SUB) + at // SUB


TOP = 13.0


def take_in(cases, use):
    def run(message, previous):
        count = message.shape[0] - 1
        back = jnp.exp2(message[count] - TOP)
        pieces, columns, height, _ = previous.shape
        for piece, j, at, b, m in tiles_of(pieces, columns, height):
            use(piece, j, at, b, message[m] * back - previous[piece, j, at, :])

    for chosen, message, previous in cases:
        pl.when(chosen)(functools.partial(run, message, previous))


def ends_of_ring():
    here = lax.axis_index("seg")
    return here == lax.axis_size("seg") - 1, here == 0


def propagate_kernel(pieces, index, first, last, final, *refs):
    refs = list(refs)
    take = lambda count: [refs.pop(0) for _ in range(count)]
    velocity = take(pieces)
    depth, _, columns, height, _ = velocity[0].shape
    rows, count = pieces * height, pieces * columns * height // SUB
    if first:
        previous = take(pieces)
    else:
        previous, missed, message = take(3)
        wrapped = None if last else take(1)[0]
        (start,) = take(1)
    (sent,) = take(1)
    error = None if final else take(1)[0]
    ping, pong = refs
    at_last, at_first = ends_of_ring()

    @pl.when(at_last if last else jnp.logical_not(at_last))
    def _():
        def use(piece, j, at, b, value):
            start[piece, j, at, :] = value
            place(ping, rows, j, b, value)

        if first:
            for piece, j, at, b, m in tiles_of(pieces, columns, height):
                place(ping, rows, j, b, previous[piece][index, j, at, :])
        elif last:
            take_in([(at_last, message, previous)], use)
        else:
            take_in([(at_first, wrapped, previous), (jnp.logical_not(at_first), message, previous)], use)

        done = advance(velocity, ping, pong, pieces)
        largest = None
        for piece, j, at, b, m in tiles_of(pieces, columns, height):
            value = 0.2**depth * done[j, pl.ds(SUB + SUB * b, SUB), :]
            if not first:
                value = value + missed[m]
            sent[m] = value
            size = jnp.abs(value)
            largest = size if largest is None else jnp.maximum(largest, size)
        largest = jnp.broadcast_to(jnp.max(largest, axis=(0, 1), keepdims=True), (SUB, LANE))
        power = jnp.clip(jnp.floor(jnp.log2(largest)), -100.0, 100.0)
        scale, back = jnp.exp2(TOP - power), jnp.exp2(power - TOP)
        sent[count] = power
        for m in range(count):
            value = sent[m]
            scaled = value * scale
            wide = scaled * 8193.0
            short = wide - (wide - scaled)
            sent[m] = short
            if not final:
                error[m] = short * back - value


@functools.partial(jax.jit, static_argnames=("index", "last", "final"))
def propagate(velocity, state, index=0, last=False, final=False):
    pieces = len(velocity)
    _, _, columns, height, lane = velocity[0].shape
    count = pieces * columns * height // SUB
    first = isinstance(state, list)
    shape = lambda *s: jax.ShapeDtypeStruct(s + (lane,), jnp.float32)
    outs = ([] if first else [shape(pieces, columns, height)]) + [shape(count + 1, SUB)]
    outs = outs + ([] if final else [shape(count, SUB)])
    scratch = pltpu.VMEM((columns, pieces * height + 2 * SUB, lane), jnp.float32)
    args = [*velocity, *state]
    return pl.pallas_call(
        functools.partial(propagate_kernel, pieces, index, first, last, final),
        out_shape=outs,
        in_specs=[VMEM] * len(args),
        out_specs=[VMEM] * len(outs),
        scratch_shapes=[scratch, scratch],
        compiler_params=pltpu.CompilerParams(vmem_limit_bytes=16 << 20),
        name="propagate_last" if last else "propagate",
    )(*args)


def residual_kernel(message, wrapped, previous, previous_last, *outs):
    def use(piece, j, at, b, value):
        outs[piece][0, j, at, :] = value

    at_last, at_first = ends_of_ring()
    rest = jnp.logical_not(jnp.logical_or(at_last, at_first))
    cases = [(at_last, message, previous_last), (at_first, wrapped, previous), (rest, message, previous)]
    take_in(cases, use)


@jax.jit
def last_residual(*state):
    pieces, columns, height, lane = state[2].shape
    return pl.pallas_call(
        residual_kernel,
        out_shape=[jax.ShapeDtypeStruct((1, columns, height, lane), jnp.float32)] * pieces,
        in_specs=[VMEM] * len(state),
        out_specs=[VMEM] * pieces,
        compiler_params=pltpu.CompilerParams(vmem_limit_bytes=16 << 20),
        name="residual",
    )(*state)


def rows_kernel(pieces, index, *refs):
    velocity, previous, (moved, ping, pong) = refs[:pieces], refs[pieces : 2 * pieces], refs[2 * pieces :]
    depth, _, columns, height, _ = velocity[0].shape
    for piece, j, at, b, _ in tiles_of(pieces, columns, height):
        place(ping, pieces * height, j, b, previous[piece][index, j, at, :])
    done = advance(velocity, ping, pong, pieces)
    for piece, j, at, b, _ in tiles_of(1, columns, height):
        moved[0, j, at, :] = 0.2**depth * done[j, pl.ds(SUB + SUB * b, SUB), :]


@functools.partial(jax.jit, static_argnames=("index",))
def propagate_rows(velocity, state, index):
    pieces = len(velocity)
    _, _, columns, height, lane = velocity[0].shape
    scratch = pltpu.VMEM((columns, pieces * height + 2 * SUB, lane), jnp.float32)
    return pl.pallas_call(
        functools.partial(rows_kernel, pieces, index),
        out_shape=jax.ShapeDtypeStruct((1, columns, height, lane), jnp.float32),
        in_specs=[VMEM] * (2 * pieces),
        out_specs=VMEM,
        scratch_shapes=[scratch, scratch],
        compiler_params=pltpu.CompilerParams(vmem_limit_bytes=16 << 20),
        name="propagate_rows",
    )(*velocity, *state)


def gram_kernel(share, *refs):
    residual, (gram, lines) = refs[:-2], refs[-2:]
    count = len(residual)
    _, columns, height, _ = residual[0].shape
    base = lax.axis_index("slab") * share
    sums = {}
    for j in range(columns):
        for at in range(0, height, SUB):
            values = [r[0, j, pl.ds(at, SUB), :] for r in residual]
            for p in range(count):
                for q in range(p + 1):
                    term = values[p] * values[q]
                    sums[p, q] = term if (p, q) not in sums else sums[p, q] + term
    for (p, q), total in sums.items():
        line = jnp.sum(total, axis=0, keepdims=True)
        a, b = lax.rem(base + p, count), lax.rem(base + q, count)
        lines[pl.ds(a * count + b, 1), :] = line
        if p != q:
            lines[pl.ds(b * count + a, 1), :] = line
    totals = jnp.where(diagonal(count), jnp.sum(lines[...], axis=1, keepdims=True), 0.0)
    gram[...] = jnp.broadcast_to(jnp.sum(totals, axis=0, keepdims=True), gram.shape)


def diagonal(count):
    shape = (count * count, LANE)
    return lax.broadcasted_iota(jnp.int32, shape, 0) == lax.broadcasted_iota(jnp.int32, shape, 1)


def local_gram(share, residual, copies):
    count = len(residual)
    return pl.pallas_call(
        functools.partial(gram_kernel, share),
        out_shape=jax.ShapeDtypeStruct((copies, LANE), jnp.float32),
        in_specs=[VMEM] * count,
        out_specs=VMEM,
        scratch_shapes=[pltpu.VMEM((count * count, LANE), jnp.float32)],
        compiler_params=pltpu.CompilerParams(vmem_limit_bytes=16 << 20),
        name="gram",
    )(*residual)


def solve_kernel(share, gram, *refs):
    residual, out = refs[:-1], refs[-1]
    count, columns, height, lane = out.shape
    line = jnp.broadcast_to(jnp.sum(gram[...], axis=0, keepdims=True), (count * count, lane))
    total = jnp.sum(jnp.where(diagonal(count), line, 0.0), axis=1, keepdims=True)
    entry = lambda a, b: total[a * count + b : a * count + b + 1, :]
    lower, inverse = {}, {}
    for a in range(count):
        for b in range(a + 1):
            value = entry(a, b)
            for k in range(b):
                value = value - lower[a, k] * lower[b, k]
            lower[a, b] = jnp.sqrt(value) if a == b else value / lower[b, b]
    for a in range(count):
        inverse[a, a] = 1.0 / lower[a, a]
        for b in range(a):
            value = lower[a, b] * inverse[b, b]
            for k in range(b + 1, a):
                value = value + lower[a, k] * inverse[k, b]
            inverse[a, b] = -value / lower[a, a]
    factors = {at: jnp.broadcast_to(value, (SUB, lane)) for at, value in inverse.items()}

    def finish(place):
        for j in range(columns):
            for at in range(0, height, SUB):
                values = [residual[place[a]][0, j, pl.ds(at, SUB), :] for a in range(count)]
                for a in range(count):
                    value = factors[a, 0] * values[0]
                    for b in range(1, a + 1):
                        value = value + factors[a, b] * values[b]
                    out[a, j, pl.ds(at, SUB), :] = value

    base = lax.axis_index("slab") * share
    for turn in range(0, count, share or count):
        pl.when(base == turn)(functools.partial(finish, [(a - turn) % count for a in range(count)]))


def solved(share, gram, residual):
    count, (_, columns, height, lane) = len(residual), residual[0].shape
    return pl.pallas_call(
        functools.partial(solve_kernel, share),
        out_shape=jax.ShapeDtypeStruct((count, columns, height, lane), jnp.float32),
        in_specs=[VMEM] * (1 + count),
        out_specs=VMEM,
        compiler_params=pltpu.CompilerParams(vmem_limit_bytes=16 << 20),
        name="solve",
    )(gram, *residual)


def from_slab(value, distance):
    size = lax.axis_size("slab")
    return lax.ppermute(value, "slab", [((i + distance) % size, i) for i in range(size)])


def to_next(value, segments=None):
    size = lax.axis_size("seg")
    return lax.ppermute(value, "seg", [(i, (i + 1) % size) for i in segments or range(size)])


def sent_short(message, segments=None):
    return to_next(message.astype(jnp.float16), segments).astype(jnp.float32)


def split_vectors(vectors, velocity):
    slabs, mine = lax.axis_size("slab"), lax.axis_index("slab")
    share = vectors.shape[0] // slabs

    def part(distance):
        at = lax.rem(mine + distance, slabs) * share
        return lax.dynamic_slice_in_dim(vectors, at, share, 0)

    start, speeds = [part(0)], [velocity]
    for d in range(1, slabs):
        start.append(from_slab(part(slabs - d), d))
        speeds.append(from_slab(velocity, d))
    end = lax.axis_size("seg") - 1
    previous = [jnp.concatenate([part[i : i + 1] for part in start], 0) for i in range(share)]
    own, ends = list(previous), list(previous)
    arrived, wrapped, missed, missed_end = [[None] * share for _ in range(4)]
    for hop in range(HOPS):
        for i in range(share):
            if hop == 0:
                state_end, state = start, start
            else:
                state_end = (ends[i], missed_end[i], arrived[i])
                state = (own[i], missed[i], arrived[i], wrapped[i])
            final, index = hop + 1 == HOPS, i if hop == 0 else 0
            out_end = list(propagate(speeds, state_end, index, last=True, final=final))
            out = list(propagate(speeds, state, index, final=final))
            if hop:
                ends[i], own[i] = out_end.pop(0), out.pop(0)
            if not final:
                missed_end[i], missed[i] = out_end.pop(), out.pop()
            sent_end, sent = out_end[0], out[0]
            wrapped[i] = sent_short(sent_end, [end])
            arrived[i] = sent_short(sent, range(end))
    parts = [last_residual(arrived[i], wrapped[i], own[i], ends[i]) for i in range(share)]
    residual = []
    for d in range(slabs):
        for i in range(share):
            part_i = parts[i][(slabs - d) % slabs]
            residual.append(from_slab(part_i, d) if d else part_i)
    return share, residual


def split_rows(vectors, velocity):
    depth, height = velocity.shape[0], vectors.shape[2]

    def pieces(value):
        after = value[..., :depth, :]
        before = value[..., height - depth :, :]
        return [value, from_slab(after, 1), from_slab(before, -1)]

    speeds = pieces(velocity)
    begun = vectors
    for _ in range(HOPS):
        state = pieces(begun)
        arrived = [to_next(propagate_rows(speeds, state, i)) for i in range(vectors.shape[0])]
        begun = jnp.concatenate(arrived, 0) - begun
    return 0, [begun[i : i + 1] for i in range(vectors.shape[0])]


def shards(block, base_velocity):
    vectors, velocity = tiled(block[0]), tiled(base_velocity[0])
    even = vectors.shape[0] % lax.axis_size("slab") == 0
    share, residual = (split_vectors if even else split_rows)(vectors, velocity)
    axes = ("seg", "slab")
    gram = local_gram(share, residual, lax.axis_size("seg") * lax.axis_size("slab"))
    gram = lax.all_to_all(gram, axes, 0, 0, tiled=True)
    return untiled(solved(share, gram, residual))[None]


def solution(mesh):
    placed = (P("seg", None, "slab", None), P("seg", None, None, "slab", None))
    return jax.shard_map(
        shards, mesh=mesh, in_specs=placed, out_specs=P("seg", None, "slab", None), check_vma=False
    )
```

```python
import functools

import jax
import jax.numpy as jnp
from jax import lax
from jax.experimental import pallas as pl
from jax.experimental.pallas import tpu as pltpu
from jax.sharding import PartitionSpec as P


HOPS = 4
SUB = 8
LANE = 128
VMEM = pl.BlockSpec(memory_space=pltpu.VMEM)


def tiled(rows):
    lead, (height, width) = rows.shape[:-2], rows.shape[-2:]
    cut = rows.reshape(lead + (height, width // LANE, LANE))
    return jnp.swapaxes(cut, -3, -2)


def untiled(tiles):
    lead, (count, height, lane) = tiles.shape[:-3], tiles.shape[-3:]
    return jnp.swapaxes(tiles, -3, -2).reshape(lead + (height, count * lane))


def advance(velocity, ping, pong, pieces):
    depth, _, columns, height, _ = velocity[0].shape
    rows = pieces * height
    lane = lax.broadcasted_iota(jnp.int32, (SUB, LANE), 1)
    first, last = lane == 0, lane == LANE - 1

    def step(k, source, target):
        for b in range(rows // SUB):
            piece, at = divmod(SUB * b, height)
            rows_at = pl.ds(SUB + SUB * b, SUB)
            here = [source[j % columns, rows_at, :] for j in (-1, 0, 1)]
            for j in range(columns):
                left, centre, right = here
                west = pltpu.roll(jnp.where(last, left, centre), 1, 1)
                east = pltpu.roll(jnp.where(first, right, centre), LANE - 1, 1)
                up = source[j, pl.ds(SUB + 1 + SUB * b, SUB), :]
                down = source[j, pl.ds(SUB - 1 + SUB * b, SUB), :]
                speed_x = velocity[piece][k, 0, j, pl.ds(at, SUB), :].astype(jnp.float32)
                speed_y = velocity[piece][k, 1, j, pl.ds(at, SUB), :].astype(jnp.float32)
                carried = speed_x * (west - east) + speed_y * (down - up)
                place(target, rows, j, b, 0.9 * centre + ((west + east) + (up + down)) + 0.25 * carried)
                here = [centre, right, source[(j + 2) % columns, rows_at, :]]

    def pair(i, carry):
        step(2 * i, ping, pong)
        step(2 * i + 1, pong, ping)
        return carry

    lax.fori_loop(0, depth // 2, pair, 0)
    if depth % 2:
        step(depth - 1, ping, pong)
        return pong
    return ping


def place(ref, rows, j, b, value):
    ref[j, pl.ds(SUB + SUB * b, SUB), :] = value
    if b == 0:
        ref[j, pl.ds(SUB + rows, 1), :] = value[:1]
    if b == rows // SUB - 1:
        ref[j, pl.ds(SUB - 1, 1), :] = value[SUB - 1 :]


def tiles_of(pieces, columns, height):
    for j in range(columns):
        for b in range(pieces * height // SUB):
            piece, at = divmod(SUB * b, height)
            yield piece, j, pl.ds(at, SUB), b, (piece * columns + j) * (height // SUB) + at // SUB


TOP = 13.0


def take_in(cases, use):
    def run(message, previous):
        count = message.shape[0] - 1
        back = jnp.exp2(message[count] - TOP)
        pieces, columns, height, _ = previous.shape
        for piece, j, at, b, m in tiles_of(pieces, columns, height):
            use(piece, j, at, b, message[m] * back - previous[piece, j, at, :])

    for chosen, message, previous in cases:
        pl.when(chosen)(functools.partial(run, message, previous))


GROUP = 4


def group_size(segments):
    return GROUP if segments % GROUP == 0 else segments


def ends_of_group():
    group = group_size(lax.axis_size("seg"))
    place = lax.rem(lax.axis_index("seg"), group)
    return place == group - 1, place == 0


def propagate_kernel(pieces, index, first, last, final, *refs):
    refs = list(refs)
    take = lambda count: [refs.pop(0) for _ in range(count)]
    velocity = take(pieces)
    depth, _, columns, height, _ = velocity[0].shape
    rows, count = pieces * height, pieces * columns * height // SUB
    if first:
        previous = take(pieces)
    else:
        previous, missed, message = take(3)
        wrapped = None if last else take(1)[0]
        (start,) = take(1)
    (sent,) = take(1)
    error = None if final else take(1)[0]
    ping, pong = refs
    at_last, at_first = ends_of_group()

    @pl.when(at_last if last else jnp.logical_not(at_last))
    def _():
        def use(piece, j, at, b, value):
            start[piece, j, at, :] = value
            place(ping, rows, j, b, value)

        if first:
            for piece, j, at, b, m in tiles_of(pieces, columns, height):
                place(ping, rows, j, b, previous[piece][index, j, at, :])
        elif last:
            take_in([(at_last, message, previous)], use)
        else:
            take_in([(at_first, wrapped, previous), (jnp.logical_not(at_first), message, previous)], use)

        done = advance(velocity, ping, pong, pieces)
        largest = None
        for piece, j, at, b, m in tiles_of(pieces, columns, height):
            value = 0.2**depth * done[j, pl.ds(SUB + SUB * b, SUB), :]
            if not first:
                value = value + missed[m]
            sent[m] = value
            size = jnp.abs(value)
            largest = size if largest is None else jnp.maximum(largest, size)
        largest = jnp.broadcast_to(jnp.max(largest, axis=(0, 1), keepdims=True), (SUB, LANE))
        power = jnp.clip(jnp.floor(jnp.log2(largest)), -100.0, 100.0)
        scale, back = jnp.exp2(TOP - power), jnp.exp2(power - TOP)
        sent[count] = power
        for m in range(count):
            value = sent[m]
            scaled = value * scale
            wide = scaled * 8193.0
            short = wide - (wide - scaled)
            sent[m] = short
            if not final:
                error[m] = short * back - value


@functools.partial(jax.jit, static_argnames=("index", "last", "final"))
def propagate(velocity, state, index=0, last=False, final=False):
    pieces = len(velocity)
    _, _, columns, height, lane = velocity[0].shape
    count = pieces * columns * height // SUB
    first = isinstance(state, list)
    shape = lambda *s: jax.ShapeDtypeStruct(s + (lane,), jnp.float32)
    outs = ([] if first else [shape(pieces, columns, height)]) + [shape(count + 1, SUB)]
    outs = outs + ([] if final else [shape(count, SUB)])
    scratch = pltpu.VMEM((columns, pieces * height + 2 * SUB, lane), jnp.float32)
    args = [*velocity, *state]
    return pl.pallas_call(
        functools.partial(propagate_kernel, pieces, index, first, last, final),
        out_shape=outs,
        in_specs=[VMEM] * len(args),
        out_specs=[VMEM] * len(outs),
        scratch_shapes=[scratch, scratch],
        compiler_params=pltpu.CompilerParams(vmem_limit_bytes=16 << 20),
        name="propagate_last" if last else "propagate",
    )(*args)


def residual_kernel(message, wrapped, previous, previous_last, *outs):
    def use(piece, j, at, b, value):
        outs[piece][0, j, at, :] = value

    at_last, at_first = ends_of_group()
    rest = jnp.logical_not(jnp.logical_or(at_last, at_first))
    cases = [(at_last, message, previous_last), (at_first, wrapped, previous), (rest, message, previous)]
    take_in(cases, use)


@jax.jit
def last_residual(*state):
    pieces, columns, height, lane = state[2].shape
    return pl.pallas_call(
        residual_kernel,
        out_shape=[jax.ShapeDtypeStruct((1, columns, height, lane), jnp.float32)] * pieces,
        in_specs=[VMEM] * len(state),
        out_specs=[VMEM] * pieces,
        compiler_params=pltpu.CompilerParams(vmem_limit_bytes=16 << 20),
        name="residual",
    )(*state)


def rows_kernel(pieces, index, *refs):
    velocity, previous, (moved, ping, pong) = refs[:pieces], refs[pieces : 2 * pieces], refs[2 * pieces :]
    depth, _, columns, height, _ = velocity[0].shape
    for piece, j, at, b, _ in tiles_of(pieces, columns, height):
        place(ping, pieces * height, j, b, previous[piece][index, j, at, :])
    done = advance(velocity, ping, pong, pieces)
    for piece, j, at, b, _ in tiles_of(1, columns, height):
        moved[0, j, at, :] = 0.2**depth * done[j, pl.ds(SUB + SUB * b, SUB), :]


@functools.partial(jax.jit, static_argnames=("index",))
def propagate_rows(velocity, state, index):
    pieces = len(velocity)
    _, _, columns, height, lane = velocity[0].shape
    scratch = pltpu.VMEM((columns, pieces * height + 2 * SUB, lane), jnp.float32)
    return pl.pallas_call(
        functools.partial(rows_kernel, pieces, index),
        out_shape=jax.ShapeDtypeStruct((1, columns, height, lane), jnp.float32),
        in_specs=[VMEM] * (2 * pieces),
        out_specs=VMEM,
        scratch_shapes=[scratch, scratch],
        compiler_params=pltpu.CompilerParams(vmem_limit_bytes=16 << 20),
        name="propagate_rows",
    )(*velocity, *state)


def gram_kernel(share, *refs):
    residual, (gram, lines) = refs[:-2], refs[-2:]
    count = len(residual)
    _, columns, height, _ = residual[0].shape
    base = lax.axis_index("slab") * share
    sums = {}
    for j in range(columns):
        for at in range(0, height, SUB):
            values = [r[0, j, pl.ds(at, SUB), :] for r in residual]
            for p in range(count):
                for q in range(p + 1):
                    term = values[p] * values[q]
                    sums[p, q] = term if (p, q) not in sums else sums[p, q] + term
    for (p, q), total in sums.items():
        line = jnp.sum(total, axis=0, keepdims=True)
        a, b = lax.rem(base + p, count), lax.rem(base + q, count)
        lines[pl.ds(a * count + b, 1), :] = line
        if p != q:
            lines[pl.ds(b * count + a, 1), :] = line
    totals = jnp.where(diagonal(count), jnp.sum(lines[...], axis=1, keepdims=True), 0.0)
    gram[...] = jnp.broadcast_to(jnp.sum(totals, axis=0, keepdims=True), gram.shape)


def diagonal(count):
    shape = (count * count, LANE)
    return lax.broadcasted_iota(jnp.int32, shape, 0) == lax.broadcasted_iota(jnp.int32, shape, 1)


def local_gram(share, residual, copies):
    count = len(residual)
    return pl.pallas_call(
        functools.partial(gram_kernel, share),
        out_shape=jax.ShapeDtypeStruct((copies, LANE), jnp.float32),
        in_specs=[VMEM] * count,
        out_specs=VMEM,
        scratch_shapes=[pltpu.VMEM((count * count, LANE), jnp.float32)],
        compiler_params=pltpu.CompilerParams(vmem_limit_bytes=16 << 20),
        name="gram",
    )(*residual)


def solve_kernel(share, gram, *refs):
    residual, out = refs[:-1], refs[-1]
    count, columns, height, lane = out.shape
    line = jnp.broadcast_to(jnp.sum(gram[...], axis=0, keepdims=True), (count * count, lane))
    total = jnp.sum(jnp.where(diagonal(count), line, 0.0), axis=1, keepdims=True)
    entry = lambda a, b: total[a * count + b : a * count + b + 1, :]
    lower, inverse = {}, {}
    for a in range(count):
        for b in range(a + 1):
            value = entry(a, b)
            for k in range(b):
                value = value - lower[a, k] * lower[b, k]
            lower[a, b] = jnp.sqrt(value) if a == b else value / lower[b, b]
    for a in range(count):
        inverse[a, a] = 1.0 / lower[a, a]
        for b in range(a):
            value = lower[a, b] * inverse[b, b]
            for k in range(b + 1, a):
                value = value + lower[a, k] * inverse[k, b]
            inverse[a, b] = -value / lower[a, a]
    factors = {at: jnp.broadcast_to(value, (SUB, lane)) for at, value in inverse.items()}

    def finish(place):
        for j in range(columns):
            for at in range(0, height, SUB):
                values = [residual[place[a]][0, j, pl.ds(at, SUB), :] for a in range(count)]
                for a in range(count):
                    value = factors[a, 0] * values[0]
                    for b in range(1, a + 1):
                        value = value + factors[a, b] * values[b]
                    out[a, j, pl.ds(at, SUB), :] = value

    base = lax.axis_index("slab") * share
    for turn in range(0, count, share or count):
        pl.when(base == turn)(functools.partial(finish, [(a - turn) % count for a in range(count)]))


def solved(share, gram, residual):
    count, (_, columns, height, lane) = len(residual), residual[0].shape
    return pl.pallas_call(
        functools.partial(solve_kernel, share),
        out_shape=jax.ShapeDtypeStruct((count, columns, height, lane), jnp.float32),
        in_specs=[VMEM] * (1 + count),
        out_specs=VMEM,
        compiler_params=pltpu.CompilerParams(vmem_limit_bytes=16 << 20),
        name="solve",
    )(gram, *residual)


def from_slab(value, distance):
    size = lax.axis_size("slab")
    return lax.ppermute(value, "slab", [((i + distance) % size, i) for i in range(size)])


def to_next(value):
    size = lax.axis_size("seg")
    return lax.ppermute(value, "seg", [(i, (i + 1) % size) for i in range(size)])


def within_group(message):
    size = lax.axis_size("seg")
    group = group_size(size)
    route = [(i, i + 1 if (i + 1) % group else i + 1 - group) for i in range(size)]
    return lax.ppermute(message.astype(jnp.float16), "seg", route).astype(jnp.float32)


def to_next_group(message):
    size = lax.axis_size("seg")
    group = group_size(size)
    route = []
    for i in range(size):
        place = i % group
        target = (i + 1) % size if place == group - 1 else i + group - 1 if place == 0 else i
        route.append((i, target))
    return lax.ppermute(message.astype(jnp.float16), "seg", route).astype(jnp.float32)


def split_vectors(vectors, velocity):
    slabs, mine = lax.axis_size("slab"), lax.axis_index("slab")
    share = vectors.shape[0] // slabs

    def part(distance):
        at = lax.rem(mine + distance, slabs) * share
        return lax.dynamic_slice_in_dim(vectors, at, share, 0)

    start, speeds = [part(0)], [velocity]
    for d in range(1, slabs):
        start.append(from_slab(part(slabs - d), d))
        speeds.append(from_slab(velocity, d))
    previous = [jnp.concatenate([part[i : i + 1] for part in start], 0) for i in range(share)]
    own, ends = list(previous), list(previous)
    arrived, wrapped, missed, missed_end = [[None] * share for _ in range(4)]
    for hop in range(HOPS):
        for i in range(share):
            if hop == 0:
                state_end, state = start, start
            else:
                state_end = (ends[i], missed_end[i], arrived[i])
                state = (own[i], missed[i], arrived[i], wrapped[i])
            final, index = hop + 1 == HOPS, i if hop == 0 else 0
            out_end = list(propagate(speeds, state_end, index, last=True, final=final))
            out = list(propagate(speeds, state, index, final=final))
            if hop:
                ends[i], own[i] = out_end.pop(0), out.pop(0)
            if not final:
                missed_end[i], missed[i] = out_end.pop(), out.pop()
            sent_end, sent = out_end[0], out[0]
            wrapped[i] = to_next_group(sent_end)
            arrived[i] = within_group(sent)
    parts = [last_residual(arrived[i], wrapped[i], own[i], ends[i]) for i in range(share)]
    residual = []
    for d in range(slabs):
        for i in range(share):
            part_i = parts[i][(slabs - d) % slabs]
            residual.append(from_slab(part_i, d) if d else part_i)
    return share, residual


def split_rows(vectors, velocity):
    depth, height = velocity.shape[0], vectors.shape[2]

    def pieces(value):
        after = value[..., :depth, :]
        before = value[..., height - depth :, :]
        return [value, from_slab(after, 1), from_slab(before, -1)]

    speeds = pieces(velocity)
    begun = vectors
    for _ in range(HOPS):
        state = pieces(begun)
        arrived = [to_next(propagate_rows(speeds, state, i)) for i in range(vectors.shape[0])]
        begun = jnp.concatenate(arrived, 0) - begun
    return 0, [begun[i : i + 1] for i in range(vectors.shape[0])]


def shards(block, base_velocity):
    vectors, velocity = tiled(block[0]), tiled(base_velocity[0])
    even = vectors.shape[0] % lax.axis_size("slab") == 0
    share, residual = (split_vectors if even else split_rows)(vectors, velocity)
    axes = ("seg", "slab")
    gram = local_gram(share, residual, lax.axis_size("seg") * lax.axis_size("slab"))
    gram = lax.all_to_all(gram, axes, 0, 0, tiled=True)
    return untiled(solved(share, gram, residual))[None]


def solution(mesh):
    placed = (P("seg", None, "slab", None), P("seg", None, None, "slab", None))
    return jax.shard_map(
        shards, mesh=mesh, in_specs=placed, out_specs=P("seg", None, "slab", None), check_vma=False
    )
```

```python
import functools

import jax
import jax.numpy as jnp
from jax import lax
from jax.experimental import pallas as pl
from jax.experimental.pallas import tpu as pltpu
from jax.sharding import PartitionSpec as P

HOPS = 4
SUB = 8
LANE = 128
VMEM = pl.BlockSpec(memory_space=pltpu.VMEM)


def tiled(rows):
    lead, (height, width) = rows.shape[:-2], rows.shape[-2:]
    cut = rows.reshape(lead + (height, width // LANE, LANE))
    return jnp.swapaxes(cut, -3, -2)


def untiled(tiles):
    lead, (count, height, lane) = tiles.shape[:-3], tiles.shape[-3:]
    return jnp.swapaxes(tiles, -3, -2).reshape(lead + (height, count * lane))


def advance(velocity, ping, pong, pieces):
    depth, _, columns, height, _ = velocity[0].shape
    rows = pieces * height
    lane = lax.broadcasted_iota(jnp.int32, (SUB, LANE), 1)
    first, last = lane == 0, lane == LANE - 1

    def step(k, source, target):
        for b in range(rows // SUB):
            piece, at = divmod(SUB * b, height)
            rows_at = pl.ds(SUB + SUB * b, SUB)
            here = [source[j % columns, rows_at, :] for j in (-1, 0, 1)]
            for j in range(columns):
                left, centre, right = here
                west = pltpu.roll(jnp.where(last, left, centre), 1, 1)
                east = pltpu.roll(jnp.where(first, right, centre), LANE - 1, 1)
                up = source[j, pl.ds(SUB + 1 + SUB * b, SUB), :]
                down = source[j, pl.ds(SUB - 1 + SUB * b, SUB), :]
                speed_x = velocity[piece][k, 0, j, pl.ds(at, SUB), :].astype(jnp.float32)
                speed_y = velocity[piece][k, 1, j, pl.ds(at, SUB), :].astype(jnp.float32)
                carried = speed_x * (west - east) + speed_y * (down - up)
                place(target, rows, j, b, 0.9 * centre + ((west + east) + (up + down)) + 0.25 * carried)
                here = [centre, right, source[(j + 2) % columns, rows_at, :]]

    def pair(i, carry):
        step(2 * i, ping, pong)
        step(2 * i + 1, pong, ping)
        return carry

    lax.fori_loop(0, depth // 2, pair, 0)
    if depth % 2:
        step(depth - 1, ping, pong)
        return pong
    return ping


def place(ref, rows, j, b, value):
    ref[j, pl.ds(SUB + SUB * b, SUB), :] = value
    if b == 0:
        ref[j, pl.ds(SUB + rows, 1), :] = value[:1]
    if b == rows // SUB - 1:
        ref[j, pl.ds(SUB - 1, 1), :] = value[SUB - 1 :]


def tiles_of(pieces, columns, height):
    for j in range(columns):
        for b in range(pieces * height // SUB):
            piece, at = divmod(SUB * b, height)
            yield piece, j, pl.ds(at, SUB), b, (piece * columns + j) * (height // SUB) + at // SUB


TOP = 13.0


def scales(largest):
    largest = jnp.broadcast_to(jnp.max(largest, axis=(0, 1), keepdims=True), (SUB, LANE))
    power = jnp.clip(jnp.floor(jnp.log2(largest)), -100.0, 100.0)
    return power, jnp.exp2(TOP - power), jnp.exp2(power - TOP)


def propagate_kernel(pieces, index, first, final, *refs):
    refs = list(refs)
    take = lambda count: [refs.pop(0) for _ in range(count)]
    velocity = take(pieces)
    depth, _, columns, height, _ = velocity[0].shape
    rows, count = pieces * height, pieces * columns * height // SUB
    if first:
        previous = take(pieces)
    else:
        previous, missed, message, start = take(4)
    (sent,) = take(1)
    error = None if final else take(1)[0]
    ping, pong = refs

    most, carried = None, None
    back = None if first else jnp.exp2(message[count] - TOP)
    for piece, j, at, b, m in tiles_of(pieces, columns, height):
        if first:
            value = previous[piece][index, j, at, :]
        else:
            value = message[m] * back - previous[piece, j, at, :]
            start[piece, j, at, :] = value
            size = jnp.abs(missed[m])
            carried = size if carried is None else jnp.maximum(carried, size)
        place(ping, rows, j, b, value)
        size = jnp.abs(value)
        most = size if most is None else jnp.maximum(most, size)
    bound = 1.01 * 1.38**depth * jnp.max(most, axis=(0, 1), keepdims=True)
    if not first:
        bound = bound + jnp.max(carried, axis=(0, 1), keepdims=True)
    power, scale, back = scales(jnp.broadcast_to(bound, (SUB, LANE)))
    sent[count] = power

    done = advance(velocity, ping, pong, pieces)
    for piece, j, at, b, m in tiles_of(pieces, columns, height):
        value = 0.2**depth * done[j, pl.ds(SUB + SUB * b, SUB), :]
        if not first:
            value = value + missed[m]
        scaled = value * scale
        wide = scaled * 8193.0
        short = wide - (wide - scaled)
        sent[m] = short
        if not final:
            error[m] = short * back - value


@functools.partial(jax.jit, static_argnames=("index", "final"))
def propagate(velocity, state, index=0, final=False):
    pieces = len(velocity)
    _, _, columns, height, lane = velocity[0].shape
    count = pieces * columns * height // SUB
    first = isinstance(state, list)
    shape = lambda *s: jax.ShapeDtypeStruct(s + (lane,), jnp.float32)
    outs = ([] if first else [shape(pieces, columns, height)]) + [shape(count + 1, SUB)]
    outs = outs + ([] if final else [shape(count, SUB)])
    scratch = pltpu.VMEM((columns, pieces * height + 2 * SUB, lane), jnp.float32)
    args = [*velocity, *state]
    return pl.pallas_call(
        functools.partial(propagate_kernel, pieces, index, first, final),
        out_shape=outs,
        in_specs=[VMEM] * len(args),
        out_specs=[VMEM] * len(outs),
        scratch_shapes=[scratch, scratch],
        compiler_params=pltpu.CompilerParams(vmem_limit_bytes=16 << 20),
        name="propagate",
    )(*args)


def residual_kernel(message, previous, *outs):
    pieces, columns, height, _ = previous.shape
    back = jnp.exp2(message[message.shape[0] - 1] - TOP)
    for piece, j, at, b, m in tiles_of(pieces, columns, height):
        outs[piece][0, j, at, :] = message[m] * back - previous[piece, j, at, :]


@jax.jit
def last_residual(message, previous):
    pieces, columns, height, lane = previous.shape
    return pl.pallas_call(
        residual_kernel,
        out_shape=[jax.ShapeDtypeStruct((1, columns, height, lane), jnp.float32)] * pieces,
        in_specs=[VMEM, VMEM],
        out_specs=[VMEM] * pieces,
        compiler_params=pltpu.CompilerParams(vmem_limit_bytes=16 << 20),
        name="residual",
    )(message, previous)


def rows_kernel(pieces, index, *refs):
    velocity, previous, (moved, ping, pong) = refs[:pieces], refs[pieces : 2 * pieces], refs[2 * pieces :]
    depth, _, columns, height, _ = velocity[0].shape
    for piece, j, at, b, _ in tiles_of(pieces, columns, height):
        place(ping, pieces * height, j, b, previous[piece][index, j, at, :])
    done = advance(velocity, ping, pong, pieces)
    for piece, j, at, b, _ in tiles_of(1, columns, height):
        moved[0, j, at, :] = 0.2**depth * done[j, pl.ds(SUB + SUB * b, SUB), :]


@functools.partial(jax.jit, static_argnames=("index",))
def propagate_rows(velocity, state, index):
    pieces = len(velocity)
    _, _, columns, height, lane = velocity[0].shape
    scratch = pltpu.VMEM((columns, pieces * height + 2 * SUB, lane), jnp.float32)
    return pl.pallas_call(
        functools.partial(rows_kernel, pieces, index),
        out_shape=jax.ShapeDtypeStruct((1, columns, height, lane), jnp.float32),
        in_specs=[VMEM] * (2 * pieces),
        out_specs=VMEM,
        scratch_shapes=[scratch, scratch],
        compiler_params=pltpu.CompilerParams(vmem_limit_bytes=16 << 20),
        name="propagate_rows",
    )(*velocity, *state)


def gram_kernel(share, *refs):
    residual, (gram, lines) = refs[:-2], refs[-2:]
    count = len(residual)
    _, columns, height, _ = residual[0].shape
    base = lax.axis_index("slab") * share
    sums = {}
    for j in range(columns):
        for at in range(0, height, SUB):
            values = [r[0, j, pl.ds(at, SUB), :] for r in residual]
            for p in range(count):
                for q in range(p + 1):
                    term = values[p] * values[q]
                    sums[p, q] = term if (p, q) not in sums else sums[p, q] + term
    for (p, q), total in sums.items():
        line = jnp.sum(total, axis=0, keepdims=True)
        a, b = lax.rem(base + p, count), lax.rem(base + q, count)
        lines[pl.ds(a * count + b, 1), :] = line
        if p != q:
            lines[pl.ds(b * count + a, 1), :] = line
    totals = jnp.where(diagonal(count), jnp.sum(lines[...], axis=1, keepdims=True), 0.0)
    gram[...] = jnp.broadcast_to(jnp.sum(totals, axis=0, keepdims=True), gram.shape)


def diagonal(count):
    shape = (count * count, LANE)
    return lax.broadcasted_iota(jnp.int32, shape, 0) == lax.broadcasted_iota(jnp.int32, shape, 1)


def local_gram(share, residual, copies):
    count = len(residual)
    return pl.pallas_call(
        functools.partial(gram_kernel, share),
        out_shape=jax.ShapeDtypeStruct((copies, LANE), jnp.float32),
        in_specs=[VMEM] * count,
        out_specs=VMEM,
        scratch_shapes=[pltpu.VMEM((count * count, LANE), jnp.float32)],
        compiler_params=pltpu.CompilerParams(vmem_limit_bytes=16 << 20),
        name="gram",
    )(*residual)


def solve_kernel(share, gram, *refs):
    residual, out = refs[:-1], refs[-1]
    count, columns, height, lane = out.shape
    line = jnp.broadcast_to(jnp.sum(gram[...], axis=0, keepdims=True), (count * count, lane))
    total = jnp.sum(jnp.where(diagonal(count), line, 0.0), axis=1, keepdims=True)
    entry = lambda a, b: total[a * count + b : a * count + b + 1, :]
    lower, inverse = {}, {}
    for a in range(count):
        for b in range(a + 1):
            value = entry(a, b)
            for k in range(b):
                value = value - lower[a, k] * lower[b, k]
            lower[a, b] = jnp.sqrt(value) if a == b else value / lower[b, b]
    for a in range(count):
        inverse[a, a] = 1.0 / lower[a, a]
        for b in range(a):
            value = lower[a, b] * inverse[b, b]
            for k in range(b + 1, a):
                value = value + lower[a, k] * inverse[k, b]
            inverse[a, b] = -value / lower[a, a]
    factors = {at: jnp.broadcast_to(value, (SUB, lane)) for at, value in inverse.items()}

    def finish(place):
        for j in range(columns):
            for at in range(0, height, SUB):
                values = [residual[place[a]][0, j, pl.ds(at, SUB), :] for a in range(count)]
                for a in range(count):
                    value = factors[a, 0] * values[0]
                    for b in range(1, a + 1):
                        value = value + factors[a, b] * values[b]
                    out[a, j, pl.ds(at, SUB), :] = value

    base = lax.axis_index("slab") * share
    for turn in range(0, count, share or count):
        pl.when(base == turn)(functools.partial(finish, [(a - turn) % count for a in range(count)]))


def solved(share, gram, residual):
    count, (_, columns, height, lane) = len(residual), residual[0].shape
    return pl.pallas_call(
        functools.partial(solve_kernel, share),
        out_shape=jax.ShapeDtypeStruct((count, columns, height, lane), jnp.float32),
        in_specs=[VMEM] * (1 + count),
        out_specs=VMEM,
        compiler_params=pltpu.CompilerParams(vmem_limit_bytes=16 << 20),
        name="solve",
    )(gram, *residual)


def from_slab(value, distance):
    size = lax.axis_size("slab")
    return lax.ppermute(value, "slab", [((i + distance) % size, i) for i in range(size)])


def to_next(value):
    size = lax.axis_size("seg")
    return lax.ppermute(value, "seg", [(i, (i + 1) % size) for i in range(size)])


def sent_short(message):
    return to_next(message.astype(jnp.float16)).astype(jnp.float32)


def split_vectors(vectors, velocity):
    slabs, mine = lax.axis_size("slab"), lax.axis_index("slab")
    share = vectors.shape[0] // slabs

    def part(distance):
        at = lax.rem(mine + distance, slabs) * share
        return lax.dynamic_slice_in_dim(vectors, at, share, 0)

    start, speeds = [part(0)], [velocity]
    for d in range(1, slabs):
        start.append(from_slab(part(slabs - d), d))
        speeds.append(from_slab(velocity, d))
    previous = [jnp.concatenate([part[i : i + 1] for part in start], 0) for i in range(share)]
    arrived, missed = [None] * share, [None] * share
    for hop in range(HOPS):
        for i in range(share):
            final = hop + 1 == HOPS
            if hop == 0:
                out = list(propagate(speeds, start, i, final=final))
            else:
                out = list(propagate(speeds, (previous[i], missed[i], arrived[i]), final=final))
                previous[i] = out.pop(0)
            missed[i] = None if final else out[1]
            arrived[i] = sent_short(out[0])
    parts = [last_residual(arrived[i], previous[i]) for i in range(share)]
    residual = []
    for d in range(slabs):
        for i in range(share):
            part_i = parts[i][(slabs - d) % slabs]
            residual.append(from_slab(part_i, d) if d else part_i)
    return share, residual


def split_rows(vectors, velocity):
    depth, height = velocity.shape[0], vectors.shape[2]

    def pieces(value):
        after = value[..., :depth, :]
        before = value[..., height - depth :, :]
        return [value, from_slab(after, 1), from_slab(before, -1)]

    speeds = pieces(velocity)
    begun = vectors
    for hop in range(HOPS):
        state = pieces(begun)
        arrived = [to_next(propagate_rows(speeds, state, i)) for i in range(vectors.shape[0])]
        begun = jnp.concatenate(arrived, 0) - begun
    return 0, [begun[i : i + 1] for i in range(vectors.shape[0])]


def shards(block, base_velocity):
    vectors, velocity = tiled(block[0]), tiled(base_velocity[0])
    even = vectors.shape[0] % lax.axis_size("slab") == 0
    share, residual = (split_vectors if even else split_rows)(vectors, velocity)
    gram = local_gram(share, residual, lax.axis_size("seg") * lax.axis_size("slab"))
    gram = lax.all_to_all(gram, ("seg", "slab"), 0, 0, tiled=True)
    return untiled(solved(share, gram, residual))[None]


def solution(mesh):
    placed = (P("seg", None, "slab", None), P("seg", None, None, "slab", None))
    return jax.shard_map(
        shards, mesh=mesh, in_specs=placed, out_specs=P("seg", None, "slab", None), check_vma=False
    )
```

```python
import functools

import jax
import jax.numpy as jnp
from jax import lax
from jax.experimental import pallas as pl
from jax.experimental.pallas import tpu as pltpu
from jax.sharding import PartitionSpec as P

HOPS = 4
SUB = 8
LANE = 128
VMEM = pl.BlockSpec(memory_space=pltpu.VMEM)


def tiled(rows):
    lead, (height, width) = rows.shape[:-2], rows.shape[-2:]
    cut = rows.reshape(lead + (height, width // LANE, LANE))
    return jnp.swapaxes(cut, -3, -2)


def untiled(tiles):
    lead, (count, height, lane) = tiles.shape[:-3], tiles.shape[-3:]
    return jnp.swapaxes(tiles, -3, -2).reshape(lead + (height, count * lane))


def advance(velocity, ping, pong, pieces, unroll=False):
    depth, _, columns, height, _ = velocity[0].shape
    rows = pieces * height
    lane = lax.broadcasted_iota(jnp.int32, (SUB, LANE), 1)
    first, last = lane == 0, lane == LANE - 1

    def step(k, source, target):
        for b in range(rows // SUB):
            piece, at = divmod(SUB * b, height)
            rows_at = pl.ds(SUB + SUB * b, SUB)
            here = [source[j % columns, rows_at, :] for j in (-1, 0, 1)]
            for j in range(columns):
                left, centre, right = here
                west = pltpu.roll(jnp.where(last, left, centre), 1, 1)
                east = pltpu.roll(jnp.where(first, right, centre), LANE - 1, 1)
                up = source[j, pl.ds(SUB + 1 + SUB * b, SUB), :]
                down = source[j, pl.ds(SUB - 1 + SUB * b, SUB), :]
                speed_x = velocity[piece][k, 0, j, pl.ds(at, SUB), :].astype(jnp.float32)
                speed_y = velocity[piece][k, 1, j, pl.ds(at, SUB), :].astype(jnp.float32)
                carried = speed_x * (west - east) + speed_y * (down - up)
                place(target, rows, j, b, 0.9 * centre + ((west + east) + (up + down)) + 0.25 * carried)
                here = [centre, right, source[(j + 2) % columns, rows_at, :]]

    def pair(i, carry):
        step(2 * i, ping, pong)
        step(2 * i + 1, pong, ping)
        return carry

    if unroll:
        for i in range(depth // 2):
            pair(i, 0)
    else:
        lax.fori_loop(0, depth // 2, pair, 0)
    if depth % 2:
        step(depth - 1, ping, pong)
        return pong
    return ping


def place(ref, rows, j, b, value):
    ref[j, pl.ds(SUB + SUB * b, SUB), :] = value
    if b == 0:
        ref[j, pl.ds(SUB + rows, 1), :] = value[:1]
    if b == rows // SUB - 1:
        ref[j, pl.ds(SUB - 1, 1), :] = value[SUB - 1 :]


def tiles_of(pieces, columns, height):
    for j in range(columns):
        for b in range(pieces * height // SUB):
            piece, at = divmod(SUB * b, height)
            yield piece, j, pl.ds(at, SUB), b, (piece * columns + j) * (height // SUB) + at // SUB


TOP = 13.0


def scales(largest):
    largest = jnp.broadcast_to(jnp.max(largest, axis=(0, 1), keepdims=True), (SUB, LANE))
    power = jnp.clip(jnp.floor(jnp.log2(largest)), -100.0, 100.0)
    return power, jnp.exp2(TOP - power), jnp.exp2(power - TOP)


def propagate_kernel(pieces, index, first, final, *refs):
    refs = list(refs)
    take = lambda count: [refs.pop(0) for _ in range(count)]
    velocity = take(pieces)
    depth, _, columns, height, _ = velocity[0].shape
    rows, count = pieces * height, pieces * columns * height // SUB
    if first:
        previous = take(pieces)
    else:
        previous, missed, message, start = take(4)
    (sent,) = take(1)
    error = None if final else take(1)[0]
    ping, pong = refs

    most, carried = None, None
    back = None if first else jnp.exp2(message[count] - TOP)
    for piece, j, at, b, m in tiles_of(pieces, columns, height):
        if first:
            value = previous[piece][index, j, at, :]
        else:
            value = message[m] * back - previous[piece, j, at, :]
            start[piece, j, at, :] = value
            size = jnp.abs(missed[m])
            carried = size if carried is None else jnp.maximum(carried, size)
        place(ping, rows, j, b, value)
        size = jnp.abs(value)
        most = size if most is None else jnp.maximum(most, size)
    bound = 1.01 * 1.38**depth * jnp.max(most, axis=(0, 1), keepdims=True)
    if not first:
        bound = bound + jnp.max(carried, axis=(0, 1), keepdims=True)
    power, scale, back = scales(jnp.broadcast_to(bound, (SUB, LANE)))
    sent[count] = power

    done = advance(velocity, ping, pong, pieces, True)
    for piece, j, at, b, m in tiles_of(pieces, columns, height):
        value = 0.2**depth * done[j, pl.ds(SUB + SUB * b, SUB), :]
        if not first:
            value = value + missed[m]
        scaled = value * scale
        wide = scaled * 8193.0
        short = wide - (wide - scaled)
        sent[m] = short
        if not final:
            error[m] = short * back - value


@functools.partial(jax.jit, static_argnames=("index", "final"))
def propagate(velocity, state, index=0, final=False):
    pieces = len(velocity)
    _, _, columns, height, lane = velocity[0].shape
    count = pieces * columns * height // SUB
    first = isinstance(state, list)
    shape = lambda *s: jax.ShapeDtypeStruct(s + (lane,), jnp.float32)
    outs = ([] if first else [shape(pieces, columns, height)]) + [shape(count + 1, SUB)]
    outs = outs + ([] if final else [shape(count, SUB)])
    scratch = pltpu.VMEM((columns, pieces * height + 2 * SUB, lane), jnp.float32)
    args = [*velocity, *state]
    return pl.pallas_call(
        functools.partial(propagate_kernel, pieces, index, first, final),
        out_shape=outs,
        in_specs=[VMEM] * len(args),
        out_specs=[VMEM] * len(outs),
        scratch_shapes=[scratch, scratch],
        compiler_params=pltpu.CompilerParams(vmem_limit_bytes=16 << 20),
        name="propagate",
    )(*args)


def residual_kernel(message, previous, *outs):
    pieces, columns, height, _ = previous.shape
    back = jnp.exp2(message[message.shape[0] - 1] - TOP)
    for piece, j, at, b, m in tiles_of(pieces, columns, height):
        outs[piece][0, j, at, :] = message[m] * back - previous[piece, j, at, :]


@jax.jit
def last_residual(message, previous):
    pieces, columns, height, lane = previous.shape
    return pl.pallas_call(
        residual_kernel,
        out_shape=[jax.ShapeDtypeStruct((1, columns, height, lane), jnp.float32)] * pieces,
        in_specs=[VMEM, VMEM],
        out_specs=[VMEM] * pieces,
        compiler_params=pltpu.CompilerParams(vmem_limit_bytes=16 << 20),
        name="residual",
    )(message, previous)


def rows_kernel(pieces, index, *refs):
    velocity, previous, (moved, ping, pong) = refs[:pieces], refs[pieces : 2 * pieces], refs[2 * pieces :]
    depth, _, columns, height, _ = velocity[0].shape
    for piece, j, at, b, _ in tiles_of(pieces, columns, height):
        place(ping, pieces * height, j, b, previous[piece][index, j, at, :])
    done = advance(velocity, ping, pong, pieces)
    for piece, j, at, b, _ in tiles_of(1, columns, height):
        moved[0, j, at, :] = 0.2**depth * done[j, pl.ds(SUB + SUB * b, SUB), :]


@functools.partial(jax.jit, static_argnames=("index",))
def propagate_rows(velocity, state, index):
    pieces = len(velocity)
    _, _, columns, height, lane = velocity[0].shape
    scratch = pltpu.VMEM((columns, pieces * height + 2 * SUB, lane), jnp.float32)
    return pl.pallas_call(
        functools.partial(rows_kernel, pieces, index),
        out_shape=jax.ShapeDtypeStruct((1, columns, height, lane), jnp.float32),
        in_specs=[VMEM] * (2 * pieces),
        out_specs=VMEM,
        scratch_shapes=[scratch, scratch],
        compiler_params=pltpu.CompilerParams(vmem_limit_bytes=16 << 20),
        name="propagate_rows",
    )(*velocity, *state)


def gram_kernel(share, *refs):
    residual, (gram, lines) = refs[:-2], refs[-2:]
    count = len(residual)
    _, columns, height, _ = residual[0].shape
    base = lax.axis_index("slab") * share
    sums = {}
    for j in range(columns):
        for at in range(0, height, SUB):
            values = [r[0, j, pl.ds(at, SUB), :] for r in residual]
            for p in range(count):
                for q in range(p + 1):
                    term = values[p] * values[q]
                    sums[p, q] = term if (p, q) not in sums else sums[p, q] + term
    for (p, q), total in sums.items():
        line = jnp.sum(total, axis=0, keepdims=True)
        a, b = lax.rem(base + p, count), lax.rem(base + q, count)
        lines[pl.ds(a * count + b, 1), :] = line
        if p != q:
            lines[pl.ds(b * count + a, 1), :] = line
    totals = jnp.where(diagonal(count), jnp.sum(lines[...], axis=1, keepdims=True), 0.0)
    gram[...] = jnp.broadcast_to(jnp.sum(totals, axis=0, keepdims=True), gram.shape)


def diagonal(count):
    shape = (count * count, LANE)
    return lax.broadcasted_iota(jnp.int32, shape, 0) == lax.broadcasted_iota(jnp.int32, shape, 1)


def local_gram(share, residual, copies):
    count = len(residual)
    return pl.pallas_call(
        functools.partial(gram_kernel, share),
        out_shape=jax.ShapeDtypeStruct((copies, LANE), jnp.float32),
        in_specs=[VMEM] * count,
        out_specs=VMEM,
        scratch_shapes=[pltpu.VMEM((count * count, LANE), jnp.float32)],
        compiler_params=pltpu.CompilerParams(vmem_limit_bytes=16 << 20),
        name="gram",
    )(*residual)


def solve_kernel(share, gram, *refs):
    residual, out = refs[:-1], refs[-1]
    count, columns, height, lane = out.shape
    line = jnp.broadcast_to(jnp.sum(gram[...], axis=0, keepdims=True), (count * count, lane))
    total = jnp.sum(jnp.where(diagonal(count), line, 0.0), axis=1, keepdims=True)
    entry = lambda a, b: total[a * count + b : a * count + b + 1, :]
    lower, inverse = {}, {}
    for a in range(count):
        for b in range(a + 1):
            value = entry(a, b)
            for k in range(b):
                value = value - lower[a, k] * lower[b, k]
            lower[a, b] = jnp.sqrt(value) if a == b else value / lower[b, b]
    for a in range(count):
        inverse[a, a] = 1.0 / lower[a, a]
        for b in range(a):
            value = lower[a, b] * inverse[b, b]
            for k in range(b + 1, a):
                value = value + lower[a, k] * inverse[k, b]
            inverse[a, b] = -value / lower[a, a]
    factors = {at: jnp.broadcast_to(value, (SUB, lane)) for at, value in inverse.items()}

    def finish(place):
        for j in range(columns):
            for at in range(0, height, SUB):
                values = [residual[place[a]][0, j, pl.ds(at, SUB), :] for a in range(count)]
                for a in range(count):
                    value = factors[a, 0] * values[0]
                    for b in range(1, a + 1):
                        value = value + factors[a, b] * values[b]
                    out[a, j, pl.ds(at, SUB), :] = value

    base = lax.axis_index("slab") * share
    for turn in range(0, count, share or count):
        pl.when(base == turn)(functools.partial(finish, [(a - turn) % count for a in range(count)]))


def solved(share, gram, residual):
    count, (_, columns, height, lane) = len(residual), residual[0].shape
    return pl.pallas_call(
        functools.partial(solve_kernel, share),
        out_shape=jax.ShapeDtypeStruct((count, columns, height, lane), jnp.float32),
        in_specs=[VMEM] * (1 + count),
        out_specs=VMEM,
        compiler_params=pltpu.CompilerParams(vmem_limit_bytes=16 << 20),
        name="solve",
    )(gram, *residual)


def from_slab(value, distance):
    size = lax.axis_size("slab")
    return lax.ppermute(value, "slab", [((i + distance) % size, i) for i in range(size)])


def to_next(value):
    size = lax.axis_size("seg")
    return lax.ppermute(value, "seg", [(i, (i + 1) % size) for i in range(size)])


def sent_short(message):
    return to_next(message.astype(jnp.float16)).astype(jnp.float32)


def split_vectors(vectors, velocity):
    slabs, mine = lax.axis_size("slab"), lax.axis_index("slab")
    share = vectors.shape[0] // slabs

    def part(distance):
        at = lax.rem(mine + distance, slabs) * share
        return lax.dynamic_slice_in_dim(vectors, at, share, 0)

    start, speeds = [part(0)], [velocity]
    for d in range(1, slabs):
        start.append(from_slab(part(slabs - d), d))
        speeds.append(from_slab(velocity, d))
    previous = [jnp.concatenate([part[i : i + 1] for part in start], 0) for i in range(share)]
    arrived, missed = [None] * share, [None] * share
    for hop in range(HOPS):
        for i in range(share):
            final = hop + 1 == HOPS
            if hop == 0:
                out = list(propagate(speeds, start, i, final=final))
            else:
                out = list(propagate(speeds, (previous[i], missed[i], arrived[i]), final=final))
                previous[i] = out.pop(0)
            missed[i] = None if final else out[1]
            arrived[i] = sent_short(out[0])
    parts = [last_residual(arrived[i], previous[i]) for i in range(share)]
    residual = []
    for d in range(slabs):
        for i in range(share):
            part_i = parts[i][(slabs - d) % slabs]
            residual.append(from_slab(part_i, d) if d else part_i)
    return share, residual


def split_rows(vectors, velocity):
    depth, height = velocity.shape[0], vectors.shape[2]

    def pieces(value):
        after = value[..., :depth, :]
        before = value[..., height - depth :, :]
        return [value, from_slab(after, 1), from_slab(before, -1)]

    speeds = pieces(velocity)
    begun = vectors
    for hop in range(HOPS):
        state = pieces(begun)
        arrived = [to_next(propagate_rows(speeds, state, i)) for i in range(vectors.shape[0])]
        begun = jnp.concatenate(arrived, 0) - begun
    return 0, [begun[i : i + 1] for i in range(vectors.shape[0])]


def shards(block, base_velocity):
    vectors, velocity = tiled(block[0]), tiled(base_velocity[0])
    even = vectors.shape[0] % lax.axis_size("slab") == 0
    share, residual = (split_vectors if even else split_rows)(vectors, velocity)
    gram = local_gram(share, residual, lax.axis_size("seg") * lax.axis_size("slab"))
    gram = lax.all_to_all(gram, ("seg", "slab"), 0, 0, tiled=True)
    return untiled(solved(share, gram, residual))[None]


def solution(mesh):
    placed = (P("seg", None, "slab", None), P("seg", None, None, "slab", None))
    return jax.shard_map(
        shards, mesh=mesh, in_specs=placed, out_specs=P("seg", None, "slab", None), check_vma=False
    )
```

```python
import functools

import jax
import jax.numpy as jnp
from jax import lax
from jax.experimental import pallas as pl
from jax.experimental.pallas import tpu as pltpu
from jax.sharding import PartitionSpec as P

HOPS = 4
SUB = 8
LANE = 128
VMEM = pl.BlockSpec(memory_space=pltpu.VMEM)


def tiled(rows):
    lead, (height, width) = rows.shape[:-2], rows.shape[-2:]
    cut = rows.reshape(lead + (height, width // LANE, LANE))
    return jnp.swapaxes(cut, -3, -2)


def untiled(tiles):
    lead, (count, height, lane) = tiles.shape[:-3], tiles.shape[-3:]
    return jnp.swapaxes(tiles, -3, -2).reshape(lead + (height, count * lane))


def advance(velocity, ping, pong, pieces, unroll=False):
    depth, _, columns, height, _ = velocity[0].shape
    rows = pieces * height
    lane = lax.broadcasted_iota(jnp.int32, (SUB, LANE), 1)
    first, last = lane == 0, lane == LANE - 1

    def step(k, source, target):
        for b in range(rows // SUB):
            piece, at = divmod(SUB * b, height)
            rows_at = pl.ds(SUB + SUB * b, SUB)
            here = [source[j % columns, rows_at, :] for j in (-1, 0, 1)]
            wests = [pltpu.roll(value, 1, 1) for value in here[:2]]
            easts = [pltpu.roll(value, LANE - 1, 1) for value in here[1:]]
            for j in range(columns):
                centre, right = here[1:]
                west = jnp.where(first, wests[0], wests[1])
                east = jnp.where(last, easts[1], easts[0])
                up = source[j, pl.ds(SUB + 1 + SUB * b, SUB), :]
                down = source[j, pl.ds(SUB - 1 + SUB * b, SUB), :]
                speed_x = velocity[piece][k, 0, j, pl.ds(at, SUB), :].astype(jnp.float32)
                speed_y = velocity[piece][k, 1, j, pl.ds(at, SUB), :].astype(jnp.float32)
                carried = speed_x * (west - east) + speed_y * (down - up)
                place(target, rows, j, b, 0.9 * centre + ((west + east) + (up + down)) + 0.25 * carried)
                here = [centre, right, source[(j + 2) % columns, rows_at, :]]
                if j + 1 < columns:
                    wests = [wests[1], pltpu.roll(right, 1, 1)]
                    easts = [easts[1], pltpu.roll(here[2], LANE - 1, 1)]

    def pair(i, carry):
        step(2 * i, ping, pong)
        step(2 * i + 1, pong, ping)
        return carry

    if unroll:
        for i in range(depth // 2):
            pair(i, 0)
    else:
        lax.fori_loop(0, depth // 2, pair, 0)
    if depth % 2:
        step(depth - 1, ping, pong)
        return pong
    return ping


def place(ref, rows, j, b, value):
    ref[j, pl.ds(SUB + SUB * b, SUB), :] = value
    if b == 0:
        ref[j, pl.ds(SUB + rows, 1), :] = value[:1]
    if b == rows // SUB - 1:
        ref[j, pl.ds(SUB - 1, 1), :] = value[SUB - 1 :]


def tiles_of(pieces, columns, height):
    for j in range(columns):
        for b in range(pieces * height // SUB):
            piece, at = divmod(SUB * b, height)
            yield piece, j, pl.ds(at, SUB), b, (piece * columns + j) * (height // SUB) + at // SUB


TOP = 13.0


def scales(largest):
    largest = jnp.broadcast_to(jnp.max(largest, axis=(0, 1), keepdims=True), (SUB, LANE))
    power = jnp.clip(jnp.floor(jnp.log2(largest)), -100.0, 100.0)
    return power, jnp.exp2(TOP - power), jnp.exp2(power - TOP)


def propagate_kernel(pieces, index, first, final, *refs):
    refs = list(refs)
    take = lambda count: [refs.pop(0) for _ in range(count)]
    velocity = take(pieces)
    depth, _, columns, height, _ = velocity[0].shape
    rows, count = pieces * height, pieces * columns * height // SUB
    if first:
        previous = take(pieces)
    else:
        previous, missed, message, start = take(4)
    (sent,) = take(1)
    error = None if final else take(1)[0]
    ping, pong = refs

    most, carried = None, None
    back = None if first else jnp.exp2(message[count] - TOP)
    for piece, j, at, b, m in tiles_of(pieces, columns, height):
        if first:
            value = previous[piece][index, j, at, :]
        else:
            value = message[m] * back - previous[piece, j, at, :]
            start[piece, j, at, :] = value
            size = jnp.abs(missed[m])
            carried = size if carried is None else jnp.maximum(carried, size)
        place(ping, rows, j, b, value)
        size = jnp.abs(value)
        most = size if most is None else jnp.maximum(most, size)
    bound = 1.01 * 1.38**depth * jnp.max(most, axis=(0, 1), keepdims=True)
    if not first:
        bound = bound + jnp.max(carried, axis=(0, 1), keepdims=True)
    power, scale, back = scales(jnp.broadcast_to(bound, (SUB, LANE)))
    sent[count] = power

    done = advance(velocity, ping, pong, pieces, True)
    for piece, j, at, b, m in tiles_of(pieces, columns, height):
        value = 0.2**depth * done[j, pl.ds(SUB + SUB * b, SUB), :]
        if not first:
            value = value + missed[m]
        scaled = value * scale
        wide = scaled * 8193.0
        short = wide - (wide - scaled)
        sent[m] = short
        if not final:
            error[m] = short * back - value


@functools.partial(jax.jit, static_argnames=("index", "final"))
def propagate(velocity, state, index=0, final=False):
    pieces = len(velocity)
    _, _, columns, height, lane = velocity[0].shape
    count = pieces * columns * height // SUB
    first = isinstance(state, list)
    shape = lambda *s: jax.ShapeDtypeStruct(s + (lane,), jnp.float32)
    outs = ([] if first else [shape(pieces, columns, height)]) + [shape(count + 1, SUB)]
    outs = outs + ([] if final else [shape(count, SUB)])
    scratch = pltpu.VMEM((columns, pieces * height + 2 * SUB, lane), jnp.float32)
    args = [*velocity, *state]
    return pl.pallas_call(
        functools.partial(propagate_kernel, pieces, index, first, final),
        out_shape=outs,
        in_specs=[VMEM] * len(args),
        out_specs=[VMEM] * len(outs),
        scratch_shapes=[scratch, scratch],
        compiler_params=pltpu.CompilerParams(vmem_limit_bytes=16 << 20),
        name="propagate",
    )(*args)


def residual_kernel(message, previous, *outs):
    pieces, columns, height, _ = previous.shape
    back = jnp.exp2(message[message.shape[0] - 1] - TOP)
    for piece, j, at, b, m in tiles_of(pieces, columns, height):
        outs[piece][0, j, at, :] = message[m] * back - previous[piece, j, at, :]


@jax.jit
def last_residual(message, previous):
    pieces, columns, height, lane = previous.shape
    return pl.pallas_call(
        residual_kernel,
        out_shape=[jax.ShapeDtypeStruct((1, columns, height, lane), jnp.float32)] * pieces,
        in_specs=[VMEM, VMEM],
        out_specs=[VMEM] * pieces,
        compiler_params=pltpu.CompilerParams(vmem_limit_bytes=16 << 20),
        name="residual",
    )(message, previous)


def rows_kernel(pieces, index, *refs):
    velocity, previous, (moved, ping, pong) = refs[:pieces], refs[pieces : 2 * pieces], refs[2 * pieces :]
    depth, _, columns, height, _ = velocity[0].shape
    for piece, j, at, b, _ in tiles_of(pieces, columns, height):
        place(ping, pieces * height, j, b, previous[piece][index, j, at, :])
    done = advance(velocity, ping, pong, pieces)
    for piece, j, at, b, _ in tiles_of(1, columns, height):
        moved[0, j, at, :] = 0.2**depth * done[j, pl.ds(SUB + SUB * b, SUB), :]


@functools.partial(jax.jit, static_argnames=("index",))
def propagate_rows(velocity, state, index):
    pieces = len(velocity)
    _, _, columns, height, lane = velocity[0].shape
    scratch = pltpu.VMEM((columns, pieces * height + 2 * SUB, lane), jnp.float32)
    return pl.pallas_call(
        functools.partial(rows_kernel, pieces, index),
        out_shape=jax.ShapeDtypeStruct((1, columns, height, lane), jnp.float32),
        in_specs=[VMEM] * (2 * pieces),
        out_specs=VMEM,
        scratch_shapes=[scratch, scratch],
        compiler_params=pltpu.CompilerParams(vmem_limit_bytes=16 << 20),
        name="propagate_rows",
    )(*velocity, *state)


def gram_kernel(share, *refs):
    residual, (gram, lines) = refs[:-2], refs[-2:]
    count = len(residual)
    _, columns, height, _ = residual[0].shape
    base = lax.axis_index("slab") * share
    sums = {}
    for j in range(columns):
        for at in range(0, height, SUB):
            values = [r[0, j, pl.ds(at, SUB), :] for r in residual]
            for p in range(count):
                for q in range(p + 1):
                    term = values[p] * values[q]
                    sums[p, q] = term if (p, q) not in sums else sums[p, q] + term
    for (p, q), total in sums.items():
        line = jnp.sum(total, axis=0, keepdims=True)
        a, b = lax.rem(base + p, count), lax.rem(base + q, count)
        lines[pl.ds(a * count + b, 1), :] = line
        if p != q:
            lines[pl.ds(b * count + a, 1), :] = line
    totals = jnp.where(diagonal(count), jnp.sum(lines[...], axis=1, keepdims=True), 0.0)
    gram[...] = jnp.broadcast_to(jnp.sum(totals, axis=0, keepdims=True), gram.shape)


def diagonal(count):
    shape = (count * count, LANE)
    return lax.broadcasted_iota(jnp.int32, shape, 0) == lax.broadcasted_iota(jnp.int32, shape, 1)


def local_gram(share, residual, copies):
    count = len(residual)
    return pl.pallas_call(
        functools.partial(gram_kernel, share),
        out_shape=jax.ShapeDtypeStruct((copies, LANE), jnp.float32),
        in_specs=[VMEM] * count,
        out_specs=VMEM,
        scratch_shapes=[pltpu.VMEM((count * count, LANE), jnp.float32)],
        compiler_params=pltpu.CompilerParams(vmem_limit_bytes=16 << 20),
        name="gram",
    )(*residual)


def solve_kernel(share, gram, *refs):
    residual, out = refs[:-1], refs[-1]
    count, columns, height, lane = out.shape
    line = jnp.broadcast_to(jnp.sum(gram[...], axis=0, keepdims=True), (count * count, lane))
    total = jnp.sum(jnp.where(diagonal(count), line, 0.0), axis=1, keepdims=True)
    entry = lambda a, b: total[a * count + b : a * count + b + 1, :]
    lower, inverse = {}, {}
    for a in range(count):
        for b in range(a + 1):
            value = entry(a, b)
            for k in range(b):
                value = value - lower[a, k] * lower[b, k]
            lower[a, b] = jnp.sqrt(value) if a == b else value / lower[b, b]
    for a in range(count):
        inverse[a, a] = 1.0 / lower[a, a]
        for b in range(a):
            value = lower[a, b] * inverse[b, b]
            for k in range(b + 1, a):
                value = value + lower[a, k] * inverse[k, b]
            inverse[a, b] = -value / lower[a, a]
    factors = {at: jnp.broadcast_to(value, (SUB, lane)) for at, value in inverse.items()}

    def finish(place):
        for j in range(columns):
            for at in range(0, height, SUB):
                values = [residual[place[a]][0, j, pl.ds(at, SUB), :] for a in range(count)]
                for a in range(count):
                    value = factors[a, 0] * values[0]
                    for b in range(1, a + 1):
                        value = value + factors[a, b] * values[b]
                    out[a, j, pl.ds(at, SUB), :] = value

    base = lax.axis_index("slab") * share
    for turn in range(0, count, share or count):
        pl.when(base == turn)(functools.partial(finish, [(a - turn) % count for a in range(count)]))


def solved(share, gram, residual):
    count, (_, columns, height, lane) = len(residual), residual[0].shape
    return pl.pallas_call(
        functools.partial(solve_kernel, share),
        out_shape=jax.ShapeDtypeStruct((count, columns, height, lane), jnp.float32),
        in_specs=[VMEM] * (1 + count),
        out_specs=VMEM,
        compiler_params=pltpu.CompilerParams(vmem_limit_bytes=16 << 20),
        name="solve",
    )(gram, *residual)


def from_slab(value, distance):
    size = lax.axis_size("slab")
    return lax.ppermute(value, "slab", [((i + distance) % size, i) for i in range(size)])


def to_next(value):
    size = lax.axis_size("seg")
    return lax.ppermute(value, "seg", [(i, (i + 1) % size) for i in range(size)])


def sent_short(message):
    return to_next(message.astype(jnp.float16)).astype(jnp.float32)


def split_vectors(vectors, velocity):
    slabs, mine = lax.axis_size("slab"), lax.axis_index("slab")
    share = vectors.shape[0] // slabs

    def part(distance):
        at = lax.rem(mine + distance, slabs) * share
        return lax.dynamic_slice_in_dim(vectors, at, share, 0)

    start, speeds = [part(0)], [velocity]
    for d in range(1, slabs):
        start.append(from_slab(part(slabs - d), d))
        speeds.append(from_slab(velocity, d))
    previous = [jnp.concatenate([part[i : i + 1] for part in start], 0) for i in range(share)]
    arrived, missed = [None] * share, [None] * share
    for hop in range(HOPS):
        for i in range(share):
            final = hop + 1 == HOPS
            if hop == 0:
                out = list(propagate(speeds, start, i, final=final))
            else:
                out = list(propagate(speeds, (previous[i], missed[i], arrived[i]), final=final))
                previous[i] = out.pop(0)
            missed[i] = None if final else out[1]
            arrived[i] = sent_short(out[0])
    parts = [last_residual(arrived[i], previous[i]) for i in range(share)]
    residual = []
    for d in range(slabs):
        for i in range(share):
            part_i = parts[i][(slabs - d) % slabs]
            residual.append(from_slab(part_i, d) if d else part_i)
    return share, residual


def split_rows(vectors, velocity):
    depth, height = velocity.shape[0], vectors.shape[2]

    def pieces(value):
        after = value[..., :depth, :]
        before = value[..., height - depth :, :]
        return [value, from_slab(after, 1), from_slab(before, -1)]

    speeds = pieces(velocity)
    begun = vectors
    for hop in range(HOPS):
        state = pieces(begun)
        arrived = [to_next(propagate_rows(speeds, state, i)) for i in range(vectors.shape[0])]
        begun = jnp.concatenate(arrived, 0) - begun
    return 0, [begun[i : i + 1] for i in range(vectors.shape[0])]


def shards(block, base_velocity):
    vectors, velocity = tiled(block[0]), tiled(base_velocity[0])
    even = vectors.shape[0] % lax.axis_size("slab") == 0
    share, residual = (split_vectors if even else split_rows)(vectors, velocity)
    gram = local_gram(share, residual, lax.axis_size("seg") * lax.axis_size("slab"))
    gram = lax.all_to_all(gram, ("seg", "slab"), 0, 0, tiled=True)
    return untiled(solved(share, gram, residual))[None]


def solution(mesh):
    placed = (P("seg", None, "slab", None), P("seg", None, None, "slab", None))
    return jax.shard_map(
        shards, mesh=mesh, in_specs=placed, out_specs=P("seg", None, "slab", None), check_vma=False
    )
```

```python
import functools

import jax
import jax.numpy as jnp
from jax import lax
from jax.experimental import pallas as pl
from jax.experimental.pallas import tpu as pltpu
from jax.sharding import PartitionSpec as P

HOPS = 4
SUB = 8
LANE = 128
VMEM = pl.BlockSpec(memory_space=pltpu.VMEM)


def tiled(rows):
    lead, (height, width) = rows.shape[:-2], rows.shape[-2:]
    cut = rows.reshape(lead + (height, width // LANE, LANE))
    return jnp.swapaxes(cut, -3, -2)


def untiled(tiles):
    lead, (count, height, lane) = tiles.shape[:-3], tiles.shape[-3:]
    return jnp.swapaxes(tiles, -3, -2).reshape(lead + (height, count * lane))


def advance(velocity, ping, pong, pieces, unroll=False):
    depth, _, columns, height, _ = velocity[0].shape
    rows = pieces * height
    lane = lax.broadcasted_iota(jnp.int32, (SUB, LANE), 1)
    first, last = lane == 0, lane == LANE - 1

    def step(k, source, target):
        for b in range(rows // SUB):
            piece, at = divmod(SUB * b, height)
            rows_at = pl.ds(SUB + SUB * b, SUB)
            here = [source[j % columns, rows_at, :] for j in (-1, 0, 1)]
            wests = [pltpu.roll(value, 1, 1) for value in here[:2]]
            easts = [pltpu.roll(value, LANE - 1, 1) for value in here[1:]]
            for j in range(columns):
                centre, right = here[1:]
                west = jnp.where(first, wests[0], wests[1])
                east = jnp.where(last, easts[1], easts[0])
                up = source[j, pl.ds(SUB + 1 + SUB * b, SUB), :]
                down = source[j, pl.ds(SUB - 1 + SUB * b, SUB), :]
                speed_x = velocity[piece][k, 0, j, pl.ds(at, SUB), :].astype(jnp.float32)
                speed_y = velocity[piece][k, 1, j, pl.ds(at, SUB), :].astype(jnp.float32)
                carried = speed_x * (west - east) + speed_y * (down - up)
                place(target, rows, j, b, 0.9 * centre + ((west + east) + (up + down)) + 0.25 * carried)
                here = [centre, right, source[(j + 2) % columns, rows_at, :]]
                if j + 1 < columns:
                    wests = [wests[1], pltpu.roll(right, 1, 1)]
                    easts = [easts[1], pltpu.roll(here[2], LANE - 1, 1)]

    def pair(i, carry):
        step(2 * i, ping, pong)
        step(2 * i + 1, pong, ping)
        return carry

    if unroll:
        for i in range(depth // 2):
            pair(i, 0)
    else:
        lax.fori_loop(0, depth // 2, pair, 0)
    if depth % 2:
        step(depth - 1, ping, pong)
        return pong
    return ping


def place(ref, rows, j, b, value):
    ref[j, pl.ds(SUB + SUB * b, SUB), :] = value
    if b == 0:
        ref[j, pl.ds(SUB + rows, 1), :] = value[:1]
    if b == rows // SUB - 1:
        ref[j, pl.ds(SUB - 1, 1), :] = value[SUB - 1 :]


def tiles_of(pieces, columns, height):
    for j in range(columns):
        for b in range(pieces * height // SUB):
            piece, at = divmod(SUB * b, height)
            yield piece, j, pl.ds(at, SUB), b, (piece * columns + j) * (height // SUB) + at // SUB


TOP = 13.0


def scales(largest):
    largest = jnp.broadcast_to(jnp.max(largest, axis=(0, 1), keepdims=True), (SUB, LANE))
    power = jnp.clip(jnp.floor(jnp.log2(largest)), -100.0, 100.0)
    return power, jnp.exp2(TOP - power), jnp.exp2(power - TOP)


def propagate_kernel(pieces, index, first, final, *refs):
    refs = list(refs)
    take = lambda count: [refs.pop(0) for _ in range(count)]
    velocity = take(pieces)
    depth, _, columns, height, _ = velocity[0].shape
    rows, count = pieces * height, pieces * columns * height // SUB
    if first:
        previous = take(pieces)
    else:
        previous, missed, message, start = take(4)
    (sent,) = take(1)
    error = None if final else take(1)[0]
    ping, pong = refs

    most, carried = None, None
    back = None if first else jnp.exp2(message[count] - TOP)
    for piece, j, at, b, m in tiles_of(pieces, columns, height):
        if first:
            value = previous[piece][index, j, at, :]
        else:
            value = message[m] * back - previous[piece, j, at, :]
            start[piece, j, at, :] = value
            size = jnp.abs(missed[m])
            carried = size if carried is None else jnp.maximum(carried, size)
        place(ping, rows, j, b, value)
        size = jnp.abs(value)
        most = size if most is None else jnp.maximum(most, size)
    bound = 1.01 * 1.38**depth * jnp.max(most, axis=(0, 1), keepdims=True)
    if not first:
        bound = bound + jnp.max(carried, axis=(0, 1), keepdims=True)
    power, scale, back = scales(jnp.broadcast_to(bound, (SUB, LANE)))
    sent[count] = power

    done = advance(velocity, ping, pong, pieces, True)
    for piece, j, at, b, m in tiles_of(pieces, columns, height):
        value = 0.2**depth * done[j, pl.ds(SUB + SUB * b, SUB), :]
        if not first:
            value = value + missed[m]
        scaled = value * scale
        wide = scaled * 8193.0
        short = wide - (wide - scaled)
        sent[m] = short
        if not final:
            error[m] = short * back - value


@functools.partial(jax.jit, static_argnames=("index", "final"))
def propagate(velocity, state, index=0, final=False):
    pieces = len(velocity)
    _, _, columns, height, lane = velocity[0].shape
    count = pieces * columns * height // SUB
    first = isinstance(state, list)
    shape = lambda *s: jax.ShapeDtypeStruct(s + (lane,), jnp.float32)
    outs = ([] if first else [shape(pieces, columns, height)]) + [shape(count + 1, SUB)]
    outs = outs + ([] if final else [shape(count, SUB)])
    scratch = pltpu.VMEM((columns, pieces * height + 2 * SUB, lane), jnp.float32)
    args = [*velocity, *state]
    return pl.pallas_call(
        functools.partial(propagate_kernel, pieces, index, first, final),
        out_shape=outs,
        in_specs=[VMEM] * len(args),
        out_specs=[VMEM] * len(outs),
        scratch_shapes=[scratch, scratch],
        compiler_params=pltpu.CompilerParams(vmem_limit_bytes=16 << 20),
        name="propagate",
    )(*args)


def residual_kernel(message, previous, *outs):
    pieces, columns, height, _ = previous.shape
    back = jnp.exp2(message[message.shape[0] - 1] - TOP)
    for piece, j, at, b, m in tiles_of(pieces, columns, height):
        outs[piece][0, j, at, :] = message[m] * back - previous[piece, j, at, :]


@jax.jit
def last_residual(message, previous):
    pieces, columns, height, lane = previous.shape
    return pl.pallas_call(
        residual_kernel,
        out_shape=[jax.ShapeDtypeStruct((1, columns, height, lane), jnp.float32)] * pieces,
        in_specs=[VMEM, VMEM],
        out_specs=[VMEM] * pieces,
        compiler_params=pltpu.CompilerParams(vmem_limit_bytes=16 << 20),
        name="residual",
    )(message, previous)


def rows_kernel(pieces, index, *refs):
    velocity, previous, (moved, ping, pong) = refs[:pieces], refs[pieces : 2 * pieces], refs[2 * pieces :]
    depth, _, columns, height, _ = velocity[0].shape
    for piece, j, at, b, _ in tiles_of(pieces, columns, height):
        place(ping, pieces * height, j, b, previous[piece][index, j, at, :])
    done = advance(velocity, ping, pong, pieces)
    for piece, j, at, b, _ in tiles_of(1, columns, height):
        moved[0, j, at, :] = 0.2**depth * done[j, pl.ds(SUB + SUB * b, SUB), :]


@functools.partial(jax.jit, static_argnames=("index",))
def propagate_rows(velocity, state, index):
    pieces = len(velocity)
    _, _, columns, height, lane = velocity[0].shape
    scratch = pltpu.VMEM((columns, pieces * height + 2 * SUB, lane), jnp.float32)
    return pl.pallas_call(
        functools.partial(rows_kernel, pieces, index),
        out_shape=jax.ShapeDtypeStruct((1, columns, height, lane), jnp.float32),
        in_specs=[VMEM] * (2 * pieces),
        out_specs=VMEM,
        scratch_shapes=[scratch, scratch],
        compiler_params=pltpu.CompilerParams(vmem_limit_bytes=16 << 20),
        name="propagate_rows",
    )(*velocity, *state)


def gram_kernel(share, *refs):
    residual, (gram, lines) = refs[:-2], refs[-2:]
    count = len(residual)
    _, columns, height, _ = residual[0].shape
    base = lax.axis_index("slab") * share
    sums = {}
    for j in range(columns):
        for at in range(0, height, SUB):
            values = [r[0, j, pl.ds(at, SUB), :] for r in residual]
            for p in range(count):
                for q in range(p + 1):
                    term = values[p] * values[q]
                    sums[p, q] = term if (p, q) not in sums else sums[p, q] + term
    for (p, q), total in sums.items():
        line = jnp.sum(total, axis=0, keepdims=True)
        a, b = lax.rem(base + p, count), lax.rem(base + q, count)
        lines[pl.ds(a * count + b, 1), :] = line
        if p != q:
            lines[pl.ds(b * count + a, 1), :] = line
    totals = jnp.where(diagonal(count), jnp.sum(lines[...], axis=1, keepdims=True), 0.0)
    gram[...] = jnp.broadcast_to(jnp.sum(totals, axis=0, keepdims=True), gram.shape)


def diagonal(count):
    shape = (count * count, LANE)
    return lax.broadcasted_iota(jnp.int32, shape, 0) == lax.broadcasted_iota(jnp.int32, shape, 1)


def local_gram(share, residual, copies):
    count = len(residual)
    return pl.pallas_call(
        functools.partial(gram_kernel, share),
        out_shape=jax.ShapeDtypeStruct((copies, LANE), jnp.float32),
        in_specs=[VMEM] * count,
        out_specs=VMEM,
        scratch_shapes=[pltpu.VMEM((count * count, LANE), jnp.float32)],
        compiler_params=pltpu.CompilerParams(vmem_limit_bytes=16 << 20),
        name="gram",
    )(*residual)


def solve_kernel(share, gram, *refs):
    residual, (target, out, done) = refs[:-3], refs[-3:]
    count, columns, height, lane = out.shape
    line = jnp.broadcast_to(jnp.sum(gram[...], axis=0, keepdims=True), (count * count, lane))
    total = jnp.sum(jnp.where(diagonal(count), line, 0.0), axis=1, keepdims=True)
    entry = lambda a, b: total[a * count + b : a * count + b + 1, :]
    lower, inverse = {}, {}
    for a in range(count):
        for b in range(a + 1):
            value = entry(a, b)
            for k in range(b):
                value = value - lower[a, k] * lower[b, k]
            lower[a, b] = jnp.sqrt(value) if a == b else value / lower[b, b]
    for a in range(count):
        inverse[a, a] = 1.0 / lower[a, a]
        for b in range(a):
            value = lower[a, b] * inverse[b, b]
            for k in range(b + 1, a):
                value = value + lower[a, k] * inverse[k, b]
            inverse[a, b] = -value / lower[a, a]
    factors = {at: jnp.broadcast_to(value, (SUB, lane)) for at, value in inverse.items()}

    part = columns // done.shape[0]

    def copy(q):
        some = pl.ds(q * part, part)
        return pltpu.make_async_copy(out.at[:, some], target.at[:, some], done.at[q])

    def finish(place):
        for j in range(columns):
            for at in range(0, height, SUB):
                values = [residual[place[a]][0, j, pl.ds(at, SUB), :] for a in range(count)]
                for a in range(count):
                    value = factors[a, 0] * values[0]
                    for b in range(1, a + 1):
                        value = value + factors[a, b] * values[b]
                    out[a, j, pl.ds(at, SUB), :] = value
            if (j + 1) % part == 0:
                copy(j // part).start()
        for q in range(columns // part):
            copy(q).wait()

    base = lax.axis_index("slab") * share
    for turn in range(0, count, share or count):
        pl.when(base == turn)(functools.partial(finish, [(a - turn) % count for a in range(count)]))


def solved(share, gram, residual):
    count, (_, columns, height, lane) = len(residual), residual[0].shape
    quarters = 4 if columns % 4 == 0 else 1
    return pl.pallas_call(
        functools.partial(solve_kernel, share),
        out_shape=jax.ShapeDtypeStruct((count, columns, height, lane), jnp.float32),
        in_specs=[VMEM] * (1 + count),
        out_specs=pl.BlockSpec(memory_space=pl.ANY),
        scratch_shapes=[
            pltpu.VMEM((count, columns, height, lane), jnp.float32),
            pltpu.SemaphoreType.DMA((quarters,)),
        ],
        compiler_params=pltpu.CompilerParams(vmem_limit_bytes=16 << 20),
        name="solve",
    )(gram, *residual)


def from_slab(value, distance):
    size = lax.axis_size("slab")
    return lax.ppermute(value, "slab", [((i + distance) % size, i) for i in range(size)])


def to_next(value):
    size = lax.axis_size("seg")
    return lax.ppermute(value, "seg", [(i, (i + 1) % size) for i in range(size)])


def sent_short(message):
    return to_next(message.astype(jnp.float16)).astype(jnp.float32)


def split_vectors(vectors, velocity):
    slabs, mine = lax.axis_size("slab"), lax.axis_index("slab")
    share = vectors.shape[0] // slabs

    def part(distance):
        at = lax.rem(mine + distance, slabs) * share
        return lax.dynamic_slice_in_dim(vectors, at, share, 0)

    start, speeds = [part(0)], [velocity]
    for d in range(1, slabs):
        start.append(from_slab(part(slabs - d), d))
        speeds.append(from_slab(velocity, d))
    previous = [jnp.concatenate([part[i : i + 1] for part in start], 0) for i in range(share)]
    arrived, missed = [None] * share, [None] * share
    for hop in range(HOPS):
        for i in range(share):
            final = hop + 1 == HOPS
            if hop == 0:
                out = list(propagate(speeds, start, i, final=final))
            else:
                out = list(propagate(speeds, (previous[i], missed[i], arrived[i]), final=final))
                previous[i] = out.pop(0)
            missed[i] = None if final else out[1]
            arrived[i] = sent_short(out[0])
    parts = [last_residual(arrived[i], previous[i]) for i in range(share)]
    residual = []
    for d in range(slabs):
        for i in range(share):
            part_i = parts[i][(slabs - d) % slabs]
            residual.append(from_slab(part_i, d) if d else part_i)
    return share, residual


def split_rows(vectors, velocity):
    depth, height = velocity.shape[0], vectors.shape[2]

    def pieces(value):
        after = value[..., :depth, :]
        before = value[..., height - depth :, :]
        return [value, from_slab(after, 1), from_slab(before, -1)]

    speeds = pieces(velocity)
    begun = vectors
    for hop in range(HOPS):
        state = pieces(begun)
        arrived = [to_next(propagate_rows(speeds, state, i)) for i in range(vectors.shape[0])]
        begun = jnp.concatenate(arrived, 0) - begun
    return 0, [begun[i : i + 1] for i in range(vectors.shape[0])]


def shards(block, base_velocity):
    vectors, velocity = tiled(block[0]), tiled(base_velocity[0])
    even = vectors.shape[0] % lax.axis_size("slab") == 0
    share, residual = (split_vectors if even else split_rows)(vectors, velocity)
    gram = local_gram(share, residual, lax.axis_size("seg") * lax.axis_size("slab"))
    gram = lax.all_to_all(gram, ("seg", "slab"), 0, 0, tiled=True)
    return untiled(solved(share, gram, residual))[None]


def solution(mesh):
    placed = (P("seg", None, "slab", None), P("seg", None, None, "slab", None))
    return jax.shard_map(
        shards, mesh=mesh, in_specs=placed, out_specs=P("seg", None, "slab", None), check_vma=False
    )
```
